8 devices in a mesh: parts: 2 (over z, y), data: 4 (over x, core).
Axes of the slice: x: 2, y: 2, z: 1, core: 2. Of those that a mesh axis runs over, the one named last changes fastest.
Arguments:
- feats: bfloat16 [2048, 28], P('data')
- labels: int32 [2048], P('data')
- w_in: float32 [28, 64, 50], P(None, 'parts'), parts along dimension 1
- w_out: float32 [64, 50], P('parts'), parts along dimension 0
- mom_in: float32 [28, 64, 50], P(None, 'parts'), parts along dimension 1
- mom_out: float32 [64, 50], P('parts'), parts along dimension 0
Outputs:
- output 1: float32 [28, 64, 50], P(None, 'parts'), parts along dimension 1
- output 2: float32 [64, 50], P('parts'), parts along dimension 0
- output 3: float32 [28, 64, 50], P(None, 'parts'), parts along dimension 1
- output 4: float32 [64, 50], P('parts'), parts along dimension 0
- output 5: float32 [64], P('parts'), parts along dimension 0
There are 2 independent parts. The reference program is written for one: setup_inputs(seed, part) draws one part's arguments, and reference() takes and returns one part's arrays. A program takes and returns all parts, laid end to end along the dimension named above; an argument that names none is the same for every part.
All inputs are finite; a program needn't handle non-finite values.
Results may differ from the reference program's by a relative error of at most 0.001.
Values are sent between devices in bfloat16 or wider.
A program may use at most 1 GiB of HBM per device.

```python
import math
import jax
import jax.numpy as jnp
from jax import lax

D = 28
HIDDEN = 50
CHAINS = 32
ROWS_DEV = 512
GROUP = 4
LEAPS = 16
N_ROWS = ROWS_DEV * GROUP
STEP = 1.0 / math.sqrt(N_ROWS * (D + HIDDEN))
PRIOR_VAR = 1.0


def setup_inputs(seed: int = 0, part: int = 0) -> dict:
    key = jax.random.key(seed)
    key_mean, key_noise, key_rate, key_draw, key_part = jax.random.split(key, 5)
    centers = jax.random.normal(key_mean, (GROUP, 1, D), jnp.float32)
    noise = jax.random.normal(key_noise, (GROUP, ROWS_DEV, D), jnp.float32)
    feats = (centers + noise).reshape(N_ROWS, D).astype(jnp.bfloat16)
    rates = jax.random.randint(key_rate, (GROUP, 1), 50, 951)
    draws = jax.random.randint(key_draw, (GROUP, ROWS_DEV), 0, 1000)
    labels = (draws < rates).astype(jnp.int32).reshape(N_ROWS)
    part_key = jax.random.fold_in(key_part, part)
    key_w1, key_w2, key_m1, key_m2 = jax.random.split(part_key, 4)
    w_in = jax.random.normal(key_w1, (D, CHAINS, HIDDEN), jnp.float32) * (2.0 * D) ** -0.5
    w_out = jax.random.normal(key_w2, (CHAINS, HIDDEN), jnp.float32) * (1.5 * HIDDEN ** -0.5)
    mom_in = jax.random.normal(key_m1, (D, CHAINS, HIDDEN), jnp.float32)
    mom_out = jax.random.normal(key_m2, (CHAINS, HIDDEN), jnp.float32)
    return {'feats': feats, 'labels': labels, 'w_in': w_in, 'w_out': w_out, 'mom_in': mom_in, 'mom_out': mom_out}


def block_terms(x_rows, lab_rows, w_flat, w_out):
    pre_act = jnp.dot(x_rows, w_flat, preferred_element_type=jnp.float32).reshape(ROWS_DEV, CHAINS, HIDDEN)
    hidden_act = jnp.tanh(pre_act)
    logits = jnp.sum(hidden_act * w_out, axis=-1)
    residual = lab_rows[:, None] - jax.nn.sigmoid(logits)
    grad_out = jnp.sum(hidden_act * residual[:, :, None], axis=0)
    back_grad = (residual[:, :, None] * w_out * (1.0 - hidden_act * hidden_act)).astype(jnp.bfloat16)
    grad_in = jnp.dot(x_rows.T, back_grad.reshape(ROWS_DEV, CHAINS * HIDDEN), preferred_element_type=jnp.float32)
    return grad_in.reshape(D, CHAINS, HIDDEN), grad_out, logits


def log_post_grad(x_blocks, lab_blocks, w_in, w_out):
    w_flat = w_in.astype(jnp.bfloat16).reshape(D, CHAINS * HIDDEN)

    def row_block(acc_sum, block_in):
        grad_in, grad_out, logits = block_terms(block_in[0], block_in[1], w_flat, w_out)
        return (acc_sum[0] + grad_in, acc_sum[1] + grad_out), logits

    sums, logits = lax.scan(row_block, (jnp.zeros_like(w_in), jnp.zeros_like(w_out)), (x_blocks, lab_blocks))
    return sums[0] - w_in / PRIOR_VAR, sums[1] - w_out / PRIOR_VAR, logits


def reference(feats, labels, w_in, w_out, mom_in, mom_out):
    x_blocks = feats.reshape(GROUP, ROWS_DEV, D)
    lab_blocks = labels.astype(jnp.float32).reshape(GROUP, ROWS_DEV)
    grad_in, grad_out, logits = log_post_grad(x_blocks, lab_blocks, w_in, w_out)
    mom_in = mom_in + 0.5 * STEP * grad_in
    mom_out = mom_out + 0.5 * STEP * grad_out

    def leap_step(state_now, unused):
        pos_in, pos_out, vel_in, vel_out = state_now
        pos_in = pos_in + STEP * vel_in
        pos_out = pos_out + STEP * vel_out
        g_in, g_out, g_logits = log_post_grad(x_blocks, lab_blocks, pos_in, pos_out)
        return (pos_in, pos_out, vel_in + STEP * g_in, vel_out + STEP * g_out), None

    state_end, unused_out = lax.scan(leap_step, (w_in, w_out, mom_in, mom_out), None, length=LEAPS - 1)
    pos_in, pos_out, vel_in, vel_out = state_end
    pos_in = pos_in + STEP * vel_in
    pos_out = pos_out + STEP * vel_out
    grad_in, grad_out, logits = log_post_grad(x_blocks, lab_blocks, pos_in, pos_out)
    vel_in = vel_in + 0.5 * STEP * grad_in
    vel_out = vel_out + 0.5 * STEP * grad_out
    row_loss = jnp.sum(jax.nn.softplus(logits) - lab_blocks[:, :, None] * logits, axis=(0, 1))
    energy = row_loss + (jnp.sum(pos_in * pos_in, axis=(0, 2)) + jnp.sum(pos_out * pos_out, axis=1)) / (2.0 * PRIOR_VAR) + 0.5 * (jnp.sum(vel_in * vel_in, axis=(0, 2)) + jnp.sum(vel_out * vel_out, axis=1))
    return pos_in, pos_out, vel_in, vel_out, energy
```

```python
import functools
import math

import jax
import jax.numpy as jnp
from jax import lax
from jax.experimental import pallas as pl
from jax.experimental.pallas import tpu as pltpu
from jax.sharding import PartitionSpec as P

LEAPS = 16
PRIOR_VAR = 1.0
MESH = pl.DeviceIdType.MESH
f32 = jnp.float32
bf16 = jnp.bfloat16

GROUPS = 2
CHUNK = 256
DP = 32
HP = 64
LEAD = 2


def cat2(x):
    return jnp.concatenate([x, x], axis=1)


def kernel(dims, feats, labels, w_in, w_out, mom_in, mom_out, end_w, end_wo, end_p, end_po, end_e,
           xs, ls, wsl, psl, wos, pos, xsend, xrecv, lrecv, xf, yb, w1, w2, p1, p2,
           zb, act, slope, bgr, accw, araw, gpart, packw, packp, recvw, recvp,
           in_sem, sx, rx, sl, rl, sw, rw, sp, rp):
    D, H, rows_dev, n_rows, eps, half = dims
    G4 = 4
    NT = G4 * H // 8
    R = NT * 8
    NC = n_rows // CHUNK
    U = GROUPS * NC
    me = lax.axis_index("data")
    xi = me // 2
    ci = me % 2
    peers = {1: xi * 2 + (1 - ci), 2: (1 - xi) * 2 + ci, 3: (1 - xi) * 2 + (1 - ci)}
    mine = pl.ds(pl.multiple_of(me * 8, 8), 8)

    copies = [
        pltpu.make_async_copy(feats, xs, in_sem.at[0]),
        pltpu.make_async_copy(labels, ls, in_sem.at[1]),
        pltpu.make_async_copy(w_in.at[:, mine, :], wsl, in_sem.at[2]),
        pltpu.make_async_copy(mom_in.at[:, mine, :], psl, in_sem.at[3]),
        pltpu.make_async_copy(w_out.at[mine, :], wos, in_sem.at[4]),
        pltpu.make_async_copy(mom_out.at[mine, :], pos, in_sem.at[5]),
    ]
    for c in copies:
        c.start()
    barrier = pltpu.get_barrier_semaphore()
    for k in peers:
        pl.semaphore_signal(barrier, inc=1, device_id={"data": peers[k]}, device_id_type=MESH)

    copies[0].wait()
    copies[1].wait()
    xf[:, pl.ds(0, rows_dev)] = jnp.zeros((DP, rows_dev), f32)
    xf[pl.ds(0, D), pl.ds(0, rows_dev)] = xs[...].astype(f32)
    xsend[...] = xf[:, pl.ds(0, rows_dev)].astype(bf16)
    pl.semaphore_wait(barrier, 3)
    sends = []
    for k in (2, 3, 1):
        sends.append(pltpu.make_async_remote_copy(src_ref=xsend, dst_ref=xrecv.at[k], send_sem=sx.at[k], recv_sem=rx.at[k],
                                                  device_id={"data": peers[k]}, device_id_type=MESH))
        sends.append(pltpu.make_async_remote_copy(src_ref=ls, dst_ref=lrecv.at[k], send_sem=sl.at[k], recv_sem=rl.at[k],
                                                  device_id={"data": peers[k]}, device_id_type=MESH))
    for s in sends:
        s.start()

    for c in copies[2:]:
        c.wait()
    for ref in (w1, p1):
        ref[...] = jnp.zeros_like(ref)
    for src, dst in ((wsl, w1), (psl, p1)):
        for c in range(8):
            dst[c // 4, pl.ds(c % 4, H, stride=4), pl.ds(0, D)] = src[:, c, :].T
    for src, dst in ((wos, w2), (pos, p2)):
        t = src[...].T
        for c in range(8):
            dst[c // 4, pl.ds(c % 4, H, stride=4), :] = jnp.broadcast_to(t[:, c:c + 1], (H, 128))
    act[3] = jnp.zeros((R, CHUNK), f32)
    slope[3] = jnp.zeros((R, CHUNK), f32)
    accw[1] = jnp.zeros((R, 128), f32)
    gpart[...] = jnp.zeros((R, DP), f32)
    zb[...] = jnp.zeros_like(zb)

    def put_labels(k, lab):
        lab = lab.astype(f32)
        for j in range(rows_dev // 128):
            yb[:, pl.ds(k * rows_dev + j * 128, 128)] = jnp.broadcast_to(lab[j:j + 1, :], (8, 128))

    put_labels(0, ls[...])
    for s in sends:
        s.wait()
    for k in (1, 2, 3):
        xf[:, pl.ds(k * rows_dev, rows_dev)] = xrecv[k].astype(f32)
        put_labels(k, lrecv[k])

    def cols(u):
        return pl.ds((u % NC) * CHUNK, CHUNK)

    def grp(u):
        return (u % U) // NC

    def mm_act(u):
        return jnp.dot(w1[grp(u), pl.ds(0, R), :], xf[:, cols(u)], preferred_element_type=f32)

    def mm_grad(u):
        return lax.dot_general(bgr[u % 2], xf[:, cols(u)], (((1,), (1,)), ((), ())), preferred_element_type=f32)

    def resid(u):
        return yb[:, cols(u)] - jax.nn.sigmoid(zb[grp(u), :, cols(u)])

    def forward(u, pre):
        g, s = grp(u), u % 4
        z = None
        for h in range(NT):
            rows = pl.ds(h * 8, 8)
            wo = cat2(w2[g, rows, :])
            a = jnp.tanh(pre[h * 8:(h + 1) * 8, :])
            t = a * wo
            z = t if z is None else z + t
            act[s, rows, :] = a
            slope[s, rows, :] = wo - t * a
        zb[g, :, cols(u)] = z + pltpu.roll(z, 4, 0)

    def backward(u, r):
        g, s = grp(u), u % 4
        for h in range(NT):
            rows = pl.ds(h * 8, 8)
            ra = r * act[s, rows, :]
            ra = ra[:, :128] + ra[:, 128:]
            if u % NC == 0:
                accw[g, rows, :] = ra
            else:
                accw[g, rows, :] += ra
            bgr[u % 2, rows, :] = r * slope[s, rows, :]

    def update(g, grad, e, f):
        rows = pl.ds(0, R)
        w = w1[g, rows, :]
        p = p1[g, rows, :] + e * (grad - w / PRIOR_VAR)
        p1[g, rows, :] = p
        w1[g, rows, :] = w + f * p
        gw = jnp.sum(accw[g], axis=1, keepdims=True)
        w = w2[g, rows, :]
        p = p2[g, rows, :] + e * (gw - w / PRIOR_VAR)
        p2[g, rows, :] = p
        w2[g, rows, :] = w + f * p

    def slots(first, final, e_prev, f_prev, e_now, f_now, after_first=None):
        ahead = {}
        grad = None
        for s in range(U):
            if not (final and s + LEAD >= U):
                ahead[s + LEAD] = mm_act(s + LEAD)
            u = (s - 1) % U
            r = resid(u)
            forward(s, araw[s] if s < LEAD else ahead.pop(s))
            backward(u, r)
            g = mm_grad(u)
            if s == 0:
                update(1, gpart[...] + g, e_prev, f_prev)
                if after_first is not None:
                    after_first()
            else:
                grad = g if grad is None else grad + g
                if s == NC:
                    update(0, grad, e_now, f_now)
                    grad = None
        return ahead, grad

    for k in range(LEAD):
        araw[k] = mm_act(k)

    def step(i, carry):
        e_prev = jnp.where(i == 0, 0.0, jnp.where(i == 1, half, eps))
        f_prev = jnp.where(i == 0, 0.0, eps)
        e_now = jnp.where(i == 0, half, eps)
        ahead, grad = slots(False, False, e_prev, f_prev, e_now, eps)
        for k in range(LEAD):
            araw[k] = ahead[U + k]
        gpart[...] = grad
        return carry

    lax.fori_loop(0, LEAPS, step, 0)

    def pack(src, src_o, dst):
        for c in range(8):
            m = src[c // 4, pl.ds(c % 4, HP, stride=4), :]
            t = m.T
            dst[pl.ds(c, 16, stride=8), :] = jnp.concatenate([t[0:16], t[16:32]], axis=1)
        lane = lax.broadcasted_iota(jnp.int32, (HP, 128), 1)
        m = jnp.zeros((HP, 128), f32)
        for c in range(8):
            m = jnp.where(lane == c + 8, src_o[c // 4, pl.ds(c % 4, HP, stride=4), :], m)
        return m

    def place_out(m, dst):
        t = m.T
        dst[pl.ds(12 * 8, 8), pl.ds(64, 64)] = t[8:16, :]

    def send_pack(src, dst, ss, rs):
        out = []
        for k in (2, 3, 1):
            c = pltpu.make_async_remote_copy(src_ref=src, dst_ref=dst.at[k], send_sem=ss.at[k], recv_sem=rs.at[k],
                                             device_id={"data": peers[k]}, device_id_type=MESH)
            c.start()
            out.append(c)
        return out

    state = {}

    def send_positions():
        place_out(pack(w1, w2, packw), packw)
        state["w"] = send_pack(packw, recvw, sw, rw)

    ahead, grad = slots(False, True, eps, eps, half, 0.0, send_positions)
    r = resid(U - 1)
    backward(U - 1, r)
    update(1, grad + mm_grad(U - 1), half, 0.0)

    sub = lax.broadcasted_iota(jnp.int32, (8, 128), 0)
    lane = lax.broadcasted_iota(jnp.int32, (8, 128), 1)
    parts = []
    for g in range(GROUPS):
        z = zb[g]
        loss = jnp.maximum(z, 0.0) + jnp.log1p(jnp.exp(-jnp.abs(z))) - yb[...] * z
        rows = pl.ds(0, R)
        sq = w1[g, rows, :] * w1[g, rows, :] / PRIOR_VAR + p1[g, rows, :] * p1[g, rows, :]
        sqo = w2[g, rows, :] * w2[g, rows, :] / PRIOR_VAR + p2[g, rows, :] * p2[g, rows, :]
        sq = jnp.sum(sq.reshape(NT, 8, DP), axis=0)
        sqo = jnp.sum(sqo.reshape(NT, 8, 128), axis=0)
        quad = jnp.sum(sq, axis=1, keepdims=True) + sqo
        quad = quad + pltpu.roll(quad, 4, 0)
        parts.append(jnp.sum(loss, axis=1, keepdims=True) + 0.5 * quad)
    ener = jnp.where(sub < 4, parts[0], parts[1])
    ener = jnp.sum(jnp.where(sub == lane % 8, ener, 0.0), axis=0, keepdims=True)
    place_out(pack(p1, p2, packp), packp)
    packp[pl.ds(15 * 8, 8), pl.ds(64, 64)] = jnp.broadcast_to(ener[:, 0:64], (8, 64))
    state["p"] = send_pack(packp, recvp, sp, rp)

    lane1 = lax.broadcasted_iota(jnp.int32, (1, 128), 1)

    def unpack(q, slab, out3, out2):
        rows = pl.ds(pl.multiple_of(q * 8, 8), 8)
        for j in range(16):
            v = slab[pl.ds(j * 8, 8), :]
            out3[j, rows, :] = v[:, 0:H]
            if j + 16 < D:
                out3[j + 16, rows, :] = pltpu.roll(v, 64, 1)[:, 0:H]
            elif j + 16 == D:
                out2[rows, :] = pltpu.roll(v, 64, 1)[:, 0:H]

    def energy_of(q, slab, cur):
        v = pltpu.roll(slab[pl.ds(15 * 8, 8), :], 64, 1)[0:1, :]
        return jnp.where(lane1 // 8 == q, v, cur)

    unpack(me, packw, end_w, end_wo)
    unpack(me, packp, end_p, end_po)
    en = energy_of(me, packp, jnp.zeros((1, 128), f32))
    for c in state["w"]:
        c.wait()
    for k in (1, 2, 3):
        unpack(peers[k], recvw.at[k], end_w, end_wo)
    for c in state["p"]:
        c.wait()
    for k in (1, 2, 3):
        unpack(peers[k], recvp.at[k], end_p, end_po)
        en = energy_of(peers[k], recvp.at[k], en)
    end_e[...] = en[:, 0:32]


def solution(mesh):
    row_spec = P('data', None)
    label_spec = P('data')
    in_spec = P(None, 'parts', None)
    out_spec = P('parts', None)
    chain_spec = P('parts')

    def run_chains(feats, labels, w_in, w_out, mom_in, mom_out):
        n_rows, D = feats.shape
        H = w_in.shape[2]
        eps = 1.0 / math.sqrt(n_rows * (D + H))

        def device_body(x_rows, y_rows, wi, wo, mi, mo):
            rows_dev = x_rows.shape[0]
            NT = 4 * H // 8
            R = NT * 8
            dims = (D, H, rows_dev, n_rows, eps, 0.5 * eps)
            S = jax.ShapeDtypeStruct
            hbm = pl.BlockSpec(memory_space=pl.ANY)
            vm = pl.BlockSpec(memory_space=pltpu.VMEM)
            V = pltpu.VMEM
            dma = pltpu.SemaphoreType.DMA
            out = pl.pallas_call(
                functools.partial(kernel, dims),
                name='hmc',
                out_shape=[S(wi.shape, f32), S(wo.shape, f32), S(wi.shape, f32), S(wo.shape, f32), S((1, wo.shape[0]), f32)],
                in_specs=[hbm] * 6,
                out_specs=[vm] * 5,
                scratch_shapes=[
                    V((D, rows_dev), bf16), V((rows_dev // 128, 128), jnp.int32),
                    V((D, 8, H), f32), V((D, 8, H), f32), V((8, H), f32), V((8, H), f32),
                    V((DP, rows_dev), bf16), V((4, DP, rows_dev), bf16), V((4, rows_dev // 128, 128), jnp.int32),
                    V((DP, n_rows), f32), V((8, n_rows), f32),
                    V((GROUPS, 4 * HP, DP), f32), V((GROUPS, 4 * HP, 128), f32), V((GROUPS, 4 * HP, DP), f32), V((GROUPS, 4 * HP, 128), f32),
                    V((GROUPS, 8, n_rows), f32),
                    V((4, R, CHUNK), f32), V((4, R, CHUNK), f32), V((2, R, CHUNK), f32), V((GROUPS, R, 128), f32),
                    V((LEAD, R, CHUNK), f32), V((R, DP), f32),
                    V((128, 128), f32), V((128, 128), f32), V((4, 128, 128), f32), V((4, 128, 128), f32),
                    dma((6,)), dma((4,)), dma((4,)), dma((4,)), dma((4,)), dma((4,)), dma((4,)), dma((4,)), dma((4,)),
                ],
                compiler_params=pltpu.CompilerParams(collective_id=0, has_side_effects=True, vmem_limit_bytes=48 * 1024 * 1024),
            )(x_rows.T, y_rows.reshape(rows_dev // 128, 128), wi, wo, mi, mo)
            return out[0], out[1], out[2], out[3], out[4].reshape(-1)

        mapped = jax.shard_map(device_body, mesh=mesh, in_specs=(row_spec, label_spec, in_spec, out_spec, in_spec, out_spec),
                               out_specs=(in_spec, out_spec, in_spec, out_spec, chain_spec), check_vma=False)
        return mapped(feats, labels, w_in, w_out, mom_in, mom_out)

    return run_chains
```

```python
import functools
import math

import jax
import jax.numpy as jnp
from jax import lax
from jax.experimental import pallas as pl
from jax.experimental.pallas import tpu as pltpu
from jax.sharding import PartitionSpec as P

LEAPS = 16
PRIOR_VAR = 1.0
MESH = pl.DeviceIdType.MESH
f32 = jnp.float32
bf16 = jnp.bfloat16

GROUPS = 2
CHUNK = 256
DP = 32
HP = 64
LEAD = 2


def cat2(x):
    return jnp.concatenate([x, x], axis=1)


def kernel(dims, feats, labels, w_in, w_out, mom_in, mom_out, end_w, end_wo, end_p, end_po, end_e,
           xs, ls, wsl, psl, wos, pos, xsend, xrecv, lrecv, xf, yb, w1, w2, p1, p2,
           zb, act, slope, bgr, accw, araw, gpart, packw, packp, recvw, recvp,
           in_sem, sx, rx, sl, rl, sw, rw, sp, rp):
    D, H, rows_dev, n_rows, eps, half = dims
    G4 = 4
    NT = G4 * H // 8
    R = NT * 8
    NC = n_rows // CHUNK
    U = GROUPS * NC
    me = lax.axis_index("data")
    xi = me // 2
    ci = me % 2
    peers = {1: xi * 2 + (1 - ci), 2: (1 - xi) * 2 + ci, 3: (1 - xi) * 2 + (1 - ci)}
    mine = pl.ds(pl.multiple_of(me * 8, 8), 8)

    copies = [
        pltpu.make_async_copy(feats, xs, in_sem.at[0]),
        pltpu.make_async_copy(labels, ls, in_sem.at[1]),
        pltpu.make_async_copy(w_in.at[:, mine, :], wsl, in_sem.at[2]),
        pltpu.make_async_copy(mom_in.at[:, mine, :], psl, in_sem.at[3]),
        pltpu.make_async_copy(w_out.at[mine, :], wos, in_sem.at[4]),
        pltpu.make_async_copy(mom_out.at[mine, :], pos, in_sem.at[5]),
    ]
    for c in copies:
        c.start()
    barrier = pltpu.get_barrier_semaphore()
    for k in peers:
        pl.semaphore_signal(barrier, inc=1, device_id={"data": peers[k]}, device_id_type=MESH)

    copies[0].wait()
    copies[1].wait()
    xf[:, pl.ds(0, rows_dev)] = jnp.zeros((DP, rows_dev), f32)
    xf[pl.ds(0, D), pl.ds(0, rows_dev)] = xs[...].astype(f32)
    xsend[...] = xf[:, pl.ds(0, rows_dev)].astype(bf16)
    pl.semaphore_wait(barrier, 3)
    sends = []
    for k in (2, 3, 1):
        sends.append(pltpu.make_async_remote_copy(src_ref=xsend, dst_ref=xrecv.at[k], send_sem=sx.at[k], recv_sem=rx.at[k],
                                                  device_id={"data": peers[k]}, device_id_type=MESH))
        sends.append(pltpu.make_async_remote_copy(src_ref=ls, dst_ref=lrecv.at[k], send_sem=sl.at[k], recv_sem=rl.at[k],
                                                  device_id={"data": peers[k]}, device_id_type=MESH))
    for s in sends:
        s.start()

    for c in copies[2:]:
        c.wait()
    for ref in (w1, p1):
        ref[...] = jnp.zeros_like(ref)
    for src, dst in ((wsl, w1), (psl, p1)):
        for c in range(8):
            dst[c // 4, pl.ds(c % 4, H, stride=4), pl.ds(0, D)] = src[:, c, :].T
    for src, dst in ((wos, w2), (pos, p2)):
        t = src[...].T
        for c in range(8):
            dst[c // 4, pl.ds(c % 4, H, stride=4), :] = jnp.broadcast_to(t[:, c:c + 1], (H, 128))
    act[3] = jnp.zeros((R, CHUNK), f32)
    slope[3] = jnp.zeros((R, CHUNK), f32)
    accw[1] = jnp.zeros((R, 128), f32)
    gpart[...] = jnp.zeros((R, DP), f32)
    zb[...] = jnp.zeros_like(zb)

    def put_labels(k, lab):
        lab = lab.astype(f32)
        for j in range(rows_dev // 128):
            yb[:, pl.ds(k * rows_dev + j * 128, 128)] = jnp.broadcast_to(lab[j:j + 1, :], (8, 128))

    put_labels(0, ls[...])
    for s in sends:
        s.wait()
    for k in (1, 2, 3):
        xf[:, pl.ds(k * rows_dev, rows_dev)] = xrecv[k].astype(f32)
        put_labels(k, lrecv[k])

    def cols(u):
        return pl.ds((u % NC) * CHUNK, CHUNK)

    def grp(u):
        return (u % U) // NC

    def mm_act(u):
        return jnp.dot(w1[grp(u), pl.ds(0, R), :], xf[:, cols(u)], preferred_element_type=f32)

    def mm_grad(u):
        return lax.dot_general(bgr[u % 2], xf[:, cols(u)], (((1,), (1,)), ((), ())), preferred_element_type=f32)

    def resid(u):
        return yb[:, cols(u)] - jax.nn.sigmoid(zb[grp(u), :, cols(u)])

    def forward(u, pre):
        g, s = grp(u), u % 4
        z = None
        for h in range(NT):
            rows = pl.ds(h * 8, 8)
            wo = cat2(w2[g, rows, :])
            a = jnp.tanh(pre[h * 8:(h + 1) * 8, :])
            t = a * wo
            z = t if z is None else z + t
            act[s, rows, :] = a
            slope[s, rows, :] = wo - t * a
        zb[g, :, cols(u)] = z + pltpu.roll(z, 4, 0)

    def backward(u, r):
        g, s = grp(u), u % 4
        for h in range(NT):
            rows = pl.ds(h * 8, 8)
            ra = r * act[s, rows, :]
            ra = ra[:, :128] + ra[:, 128:]
            if u % NC == 0:
                accw[g, rows, :] = ra
            else:
                accw[g, rows, :] += ra
            bgr[u % 2, rows, :] = r * slope[s, rows, :]

    def update(g, grad, e, f):
        rows = pl.ds(0, R)
        w = w1[g, rows, :]
        p = p1[g, rows, :] + e * (grad - w / PRIOR_VAR)
        p1[g, rows, :] = p
        w1[g, rows, :] = w + f * p
        gw = jnp.sum(accw[g], axis=1, keepdims=True)
        w = w2[g, rows, :]
        p = p2[g, rows, :] + e * (gw - w / PRIOR_VAR)
        p2[g, rows, :] = p
        w2[g, rows, :] = w + f * p

    def slots(first, final, e_prev, f_prev, e_now, f_now, after_first=None):
        ahead = {}
        grad = None
        for s in range(U):
            if not (final and s + LEAD >= U):
                ahead[s + LEAD] = mm_act(s + LEAD)
            u = (s - 1) % U
            r = resid(u)
            forward(s, araw[s] if s < LEAD else ahead.pop(s))
            backward(u, r)
            g = mm_grad(u)
            if s == 0:
                update(1, gpart[...] + g, e_prev, f_prev)
                if after_first is not None:
                    after_first()
            else:
                grad = g if grad is None else grad + g
                if s == NC:
                    update(0, grad, e_now, f_now)
                    grad = None
        return ahead, grad

    for k in range(LEAD):
        araw[k] = mm_act(k)

    def step(i, carry):
        e_prev = jnp.where(i == 0, 0.0, jnp.where(i == 1, half, eps))
        f_prev = jnp.where(i == 0, 0.0, eps)
        e_now = jnp.where(i == 0, half, eps)
        ahead, grad = slots(False, False, e_prev, f_prev, e_now, eps)
        for k in range(LEAD):
            araw[k] = ahead[U + k]
        gpart[...] = grad
        return carry

    lax.fori_loop(0, LEAPS, step, 0)

    def pack(src, src_o, dst):
        for c in range(8):
            m = src[c // 4, pl.ds(c % 4, HP, stride=4), :]
            t = m.T
            dst[pl.ds(c, 16, stride=8), :] = jnp.concatenate([t[0:16], t[16:32]], axis=1)
        lane = lax.broadcasted_iota(jnp.int32, (HP, 128), 1)
        m = jnp.zeros((HP, 128), f32)
        for c in range(8):
            m = jnp.where(lane == c + 8, src_o[c // 4, pl.ds(c % 4, HP, stride=4), :], m)
        return m

    def place_out(m, dst):
        t = m.T
        dst[pl.ds(12 * 8, 8), pl.ds(64, 64)] = t[8:16, :]

    def send_pack(src, dst, ss, rs):
        out = []
        for k in (2, 3, 1):
            c = pltpu.make_async_remote_copy(src_ref=src, dst_ref=dst.at[k], send_sem=ss.at[k], recv_sem=rs.at[k],
                                             device_id={"data": peers[k]}, device_id_type=MESH)
            c.start()
            out.append(c)
        return out

    state = {}

    def send_positions():
        place_out(pack(w1, w2, packw), packw)
        state["w"] = send_pack(packw, recvw, sw, rw)

    ahead, grad = slots(False, True, eps, eps, half, 0.0, send_positions)
    r = resid(U - 1)
    backward(U - 1, r)
    update(1, grad + mm_grad(U - 1), half, 0.0)

    sub = lax.broadcasted_iota(jnp.int32, (8, 128), 0)
    lane = lax.broadcasted_iota(jnp.int32, (8, 128), 1)
    parts = []
    for g in range(GROUPS):
        z = zb[g]
        loss = jnp.maximum(z, 0.0) + jnp.log1p(jnp.exp(-jnp.abs(z))) - yb[...] * z
        rows = pl.ds(0, R)
        sq = w1[g, rows, :] * w1[g, rows, :] / PRIOR_VAR + p1[g, rows, :] * p1[g, rows, :]
        sqo = w2[g, rows, :] * w2[g, rows, :] / PRIOR_VAR + p2[g, rows, :] * p2[g, rows, :]
        sq = jnp.sum(sq.reshape(NT, 8, DP), axis=0)
        sqo = jnp.sum(sqo.reshape(NT, 8, 128), axis=0)
        quad = jnp.sum(sq, axis=1, keepdims=True) + sqo
        quad = quad + pltpu.roll(quad, 4, 0)
        parts.append(jnp.sum(loss, axis=1, keepdims=True) + 0.5 * quad)
    ener = jnp.where(sub < 4, parts[0], parts[1])
    ener = jnp.sum(jnp.where(sub == lane % 8, ener, 0.0), axis=0, keepdims=True)
    place_out(pack(p1, p2, packp), packp)
    packp[pl.ds(15 * 8, 8), pl.ds(64, 64)] = jnp.broadcast_to(ener[:, 0:64], (8, 64))
    state["p"] = send_pack(packp, recvp, sp, rp)

    lane1 = lax.broadcasted_iota(jnp.int32, (1, 128), 1)

    def unpack(q, slab, out3, out2):
        rows = pl.ds(pl.multiple_of(q * 8, 8), 8)
        for j in range(16):
            v = slab[pl.ds(j * 8, 8), :]
            out3[j, rows, :] = v[:, 0:H]
            if j + 16 < D:
                out3[j + 16, rows, :] = pltpu.roll(v, 64, 1)[:, 0:H]
            elif j + 16 == D:
                out2[rows, :] = pltpu.roll(v, 64, 1)[:, 0:H]

    def energy_of(q, slab, cur):
        v = pltpu.roll(slab[pl.ds(15 * 8, 8), :], 64, 1)[0:1, :]
        return jnp.where(lane1 // 8 == q, v, cur)

    unpack(me, packw, end_w, end_wo)
    unpack(me, packp, end_p, end_po)
    en = energy_of(me, packp, jnp.zeros((1, 128), f32))
    for c in state["w"]:
        c.wait()
    for k in (1, 2, 3):
        unpack(peers[k], recvw.at[k], end_w, end_wo)
    for c in state["p"]:
        c.wait()
    for k in (1, 2, 3):
        unpack(peers[k], recvp.at[k], end_p, end_po)
        en = energy_of(peers[k], recvp.at[k], en)
    end_e[...] = en[:, 0:32]


def store_kernel(*refs):
    sems = refs[-1]
    copies = [pltpu.make_async_copy(refs[i], refs[5 + i], sems.at[i]) for i in range(5)]
    for c in copies:
        c.start()
    for c in copies:
        c.wait()


def solution(mesh):
    row_spec = P('data', None)
    label_spec = P('data')
    in_spec = P(None, 'parts', None)
    out_spec = P('parts', None)
    chain_spec = P('parts')

    def run_chains(feats, labels, w_in, w_out, mom_in, mom_out):
        n_rows, D = feats.shape
        H = w_in.shape[2]
        eps = 1.0 / math.sqrt(n_rows * (D + H))

        def device_body(x_rows, y_rows, wi, wo, mi, mo):
            rows_dev = x_rows.shape[0]
            NT = 4 * H // 8
            R = NT * 8
            dims = (D, H, rows_dev, n_rows, eps, 0.5 * eps)
            S = jax.ShapeDtypeStruct
            hbm = pl.BlockSpec(memory_space=pltpu.HBM)
            vm = pl.BlockSpec(memory_space=pltpu.VMEM)
            V = pltpu.VMEM
            dma = pltpu.SemaphoreType.DMA
            out = pl.pallas_call(
                functools.partial(kernel, dims),
                name='hmc',
                out_shape=[S(wi.shape, f32), S(wo.shape, f32), S(wi.shape, f32), S(wo.shape, f32), S((1, wo.shape[0]), f32)],
                in_specs=[hbm] * 6,
                out_specs=[vm] * 5,
                scratch_shapes=[
                    V((D, rows_dev), bf16), V((rows_dev // 128, 128), jnp.int32),
                    V((D, 8, H), f32), V((D, 8, H), f32), V((8, H), f32), V((8, H), f32),
                    V((DP, rows_dev), bf16), V((4, DP, rows_dev), bf16), V((4, rows_dev // 128, 128), jnp.int32),
                    V((DP, n_rows), f32), V((8, n_rows), f32),
                    V((GROUPS, 4 * HP, DP), f32), V((GROUPS, 4 * HP, 128), f32), V((GROUPS, 4 * HP, DP), f32), V((GROUPS, 4 * HP, 128), f32),
                    V((GROUPS, 8, n_rows), f32),
                    V((4, R, CHUNK), f32), V((4, R, CHUNK), f32), V((2, R, CHUNK), f32), V((GROUPS, R, 128), f32),
                    V((LEAD, R, CHUNK), f32), V((R, DP), f32),
                    V((128, 128), f32), V((128, 128), f32), V((4, 128, 128), f32), V((4, 128, 128), f32),
                    dma((6,)), dma((4,)), dma((4,)), dma((4,)), dma((4,)), dma((4,)), dma((4,)), dma((4,)), dma((4,)),
                ],
                compiler_params=pltpu.CompilerParams(collective_id=0, has_side_effects=True, vmem_limit_bytes=48 * 1024 * 1024),
            )(*[pltpu.with_memory_space_constraint(a, pltpu.HBM) for a in (x_rows.T, y_rows.reshape(rows_dev // 128, 128), wi, wo, mi, mo)])
            out = pl.pallas_call(
                store_kernel,
                name='store',
                out_shape=[S(o.shape, o.dtype) for o in out],
                in_specs=[vm] * 5,
                out_specs=[hbm] * 5,
                scratch_shapes=[dma((5,))],
                compiler_params=pltpu.CompilerParams(vmem_limit_bytes=4 * 1024 * 1024),
            )(*out)
            return out[0], out[1], out[2], out[3], out[4].reshape(-1)

        mapped = jax.shard_map(device_body, mesh=mesh, in_specs=(row_spec, label_spec, in_spec, out_spec, in_spec, out_spec),
                               out_specs=(in_spec, out_spec, in_spec, out_spec, chain_spec), check_vma=False)
        return mapped(feats, labels, w_in, w_out, mom_in, mom_out)

    return run_chains
```

```python
import functools
import math

import jax
import jax.numpy as jnp
from jax import lax
from jax.experimental import pallas as pl
from jax.experimental.pallas import tpu as pltpu
from jax.sharding import PartitionSpec as P

LEAPS = 16
PRIOR_VAR = 1.0
MESH = pl.DeviceIdType.MESH
f32 = jnp.float32
bf16 = jnp.bfloat16

GROUPS = 2
CHUNK = 256
DP = 32
HP = 64
LEAD = 2
LAG = 2
UNROLL = 4


def cat2(x):
    return jnp.concatenate([x, x], axis=1)


def kernel(dims, feats, labels, w_in, w_out, mom_in, mom_out, end_w, end_wo, end_p, end_po, end_e,
           xs, ls, wsl, psl, wos, pos, xsend, xrecv, lrecv, xf, yb, w1, w2, p1, p2,
           zb, act, slope, bgr, accw, araw, gpart, packw, packp, recvw, recvp,
           in_sem, sx, rx, sl, rl, sw, rw, sp, rp):
    D, H, rows_dev, n_rows, eps, half = dims
    G4 = 4
    NT = G4 * H // 8
    R = NT * 8
    NC = n_rows // CHUNK
    U = GROUPS * NC
    me = lax.axis_index("data")
    xi = me // 2
    ci = me % 2
    peers = {1: xi * 2 + (1 - ci), 2: (1 - xi) * 2 + ci, 3: (1 - xi) * 2 + (1 - ci)}
    mine = pl.ds(pl.multiple_of(me * 8, 8), 8)

    copies = [
        pltpu.make_async_copy(feats, xs, in_sem.at[0]),
        pltpu.make_async_copy(labels, ls, in_sem.at[1]),
        pltpu.make_async_copy(w_in.at[:, mine, :], wsl, in_sem.at[2]),
        pltpu.make_async_copy(mom_in.at[:, mine, :], psl, in_sem.at[3]),
        pltpu.make_async_copy(w_out.at[mine, :], wos, in_sem.at[4]),
        pltpu.make_async_copy(mom_out.at[mine, :], pos, in_sem.at[5]),
    ]
    for c in copies:
        c.start()
    barrier = pltpu.get_barrier_semaphore()
    for k in peers:
        pl.semaphore_signal(barrier, inc=1, device_id={"data": peers[k]}, device_id_type=MESH)

    copies[0].wait()
    copies[1].wait()
    xf[:, pl.ds(0, rows_dev)] = jnp.zeros((DP, rows_dev), f32)
    xf[pl.ds(0, D), pl.ds(0, rows_dev)] = xs[...].astype(f32)
    xsend[...] = xf[:, pl.ds(0, rows_dev)].astype(bf16)
    pl.semaphore_wait(barrier, 3)
    sends = []
    for k in (2, 3, 1):
        sends.append(pltpu.make_async_remote_copy(src_ref=xsend, dst_ref=xrecv.at[k], send_sem=sx.at[k], recv_sem=rx.at[k],
                                                  device_id={"data": peers[k]}, device_id_type=MESH))
        sends.append(pltpu.make_async_remote_copy(src_ref=ls, dst_ref=lrecv.at[k], send_sem=sl.at[k], recv_sem=rl.at[k],
                                                  device_id={"data": peers[k]}, device_id_type=MESH))
    for s in sends:
        s.start()

    for c in copies[2:]:
        c.wait()
    for ref in (w1, p1):
        ref[...] = jnp.zeros_like(ref)
    for src, dst in ((wsl, w1), (psl, p1)):
        for c in range(8):
            dst[c // 4, pl.ds(c % 4, H, stride=4), pl.ds(0, D)] = src[:, c, :].T
    for src, dst in ((wos, w2), (pos, p2)):
        t = src[...].T
        for c in range(8):
            dst[c // 4, pl.ds(c % 4, H, stride=4), :] = jnp.broadcast_to(t[:, c:c + 1], (H, 128))
    for u in range(4 - LAG, 4):
        act[u] = jnp.zeros((R, CHUNK), f32)
        slope[u] = jnp.zeros((R, CHUNK), f32)
    accw[1] = jnp.zeros((R, 128), f32)
    gpart[...] = jnp.zeros((R, DP), f32)
    zb[...] = jnp.zeros_like(zb)

    def put_labels(k, lab):
        lab = lab.astype(f32)
        for j in range(rows_dev // 128):
            yb[:, pl.ds(k * rows_dev + j * 128, 128)] = jnp.broadcast_to(lab[j:j + 1, :], (8, 128))

    put_labels(0, ls[...])
    for s in sends:
        s.wait()
    for k in (1, 2, 3):
        xf[:, pl.ds(k * rows_dev, rows_dev)] = xrecv[k].astype(f32)
        put_labels(k, lrecv[k])

    def cols(u):
        return pl.ds((u % NC) * CHUNK, CHUNK)

    def grp(u):
        return (u % U) // NC

    def mm_act(u):
        return jnp.dot(w1[grp(u), pl.ds(0, R), :], xf[:, cols(u)], preferred_element_type=f32)

    def mm_grad(u):
        return lax.dot_general(bgr[u % 4], xf[:, cols(u)], (((1,), (1,)), ((), ())), preferred_element_type=f32)

    def resid(u):
        return yb[:, cols(u)] - jax.nn.sigmoid(zb[grp(u), :, cols(u)])

    def forward(u, pre):
        g, s = grp(u), u % 4
        z = None
        for h in range(NT):
            rows = pl.ds(h * 8, 8)
            wo = cat2(w2[g, rows, :])
            a = jnp.tanh(pre[h * 8:(h + 1) * 8, :])
            t = a * wo
            z = t if z is None else z + t
            act[s, rows, :] = a
            slope[s, rows, :] = wo - t * a
        zb[g, :, cols(u)] = z + pltpu.roll(z, 4, 0)

    def backward(u, r):
        g, s = grp(u), u % 4
        for h in range(NT):
            rows = pl.ds(h * 8, 8)
            ra = r * act[s, rows, :]
            ra = ra[:, :128] + ra[:, 128:]
            if u % NC == 0:
                accw[g, rows, :] = ra
            else:
                accw[g, rows, :] += ra
            bgr[u % 4, rows, :] = r * slope[s, rows, :]

    def update(g, grad, e, f):
        rows = pl.ds(0, R)
        w = w1[g, rows, :]
        p = p1[g, rows, :] + e * (grad - w / PRIOR_VAR)
        p1[g, rows, :] = p
        w1[g, rows, :] = w + f * p
        gw = jnp.sum(accw[g], axis=1, keepdims=True)
        w = w2[g, rows, :]
        p = p2[g, rows, :] + e * (gw - w / PRIOR_VAR)
        p2[g, rows, :] = p
        w2[g, rows, :] = w + f * p

    def slots(first, final, e_prev, f_prev, e_now, f_now, after_first=None):
        ahead = {}
        grad = None
        for s in range(U):
            if not (final and s + LEAD >= U):
                ahead[s + LEAD] = mm_act(s + LEAD)
            u = (s - LAG) % U
            r = resid(u)
            forward(s, araw[s] if s < LEAD else ahead.pop(s))
            backward(u, r)
            g = mm_grad(u)
            if s == 0:
                grad = gpart[...]
            grad = g if grad is None else grad + g
            if s == LAG - 1:
                update(1, grad, e_prev, f_prev)
                grad = None
                if after_first is not None:
                    after_first()
            elif s == NC + LAG - 1:
                update(0, grad, e_now, f_now)
                grad = None
        return ahead, grad

    for k in range(LEAD):
        araw[k] = mm_act(k)

    def step(i, carry):
        e_prev = jnp.where(i == 0, 0.0, jnp.where(i == 1, half, eps))
        f_prev = jnp.where(i == 0, 0.0, eps)
        e_now = jnp.where(i == 0, half, eps)
        ahead, grad = slots(False, False, e_prev, f_prev, e_now, eps)
        for k in range(LEAD):
            araw[k] = ahead[U + k]
        gpart[...] = grad
        return carry

    lax.fori_loop(0, LEAPS, step, 0, unroll=UNROLL)

    def pack(src, src_o, dst):
        for c in range(8):
            m = src[c // 4, pl.ds(c % 4, HP, stride=4), :]
            t = m.T
            dst[pl.ds(c, 16, stride=8), :] = jnp.concatenate([t[0:16], t[16:32]], axis=1)
        lane = lax.broadcasted_iota(jnp.int32, (HP, 128), 1)
        m = jnp.zeros((HP, 128), f32)
        for c in range(8):
            m = jnp.where(lane == c + 8, src_o[c // 4, pl.ds(c % 4, HP, stride=4), :], m)
        return m

    def place_out(m, dst):
        t = m.T
        dst[pl.ds(12 * 8, 8), pl.ds(64, 64)] = t[8:16, :]

    def send_pack(src, dst, ss, rs):
        out = []
        for k in (2, 3, 1):
            c = pltpu.make_async_remote_copy(src_ref=src, dst_ref=dst.at[k], send_sem=ss.at[k], recv_sem=rs.at[k],
                                             device_id={"data": peers[k]}, device_id_type=MESH)
            c.start()
            out.append(c)
        return out

    state = {}

    def send_positions():
        place_out(pack(w1, w2, packw), packw)
        state["w"] = send_pack(packw, recvw, sw, rw)

    ahead, grad = slots(False, True, eps, eps, half, 0.0, send_positions)
    for u in range(U - LAG, U):
        backward(u, resid(u))
        grad = grad + mm_grad(u)
    update(1, grad, half, 0.0)

    sub = lax.broadcasted_iota(jnp.int32, (8, 128), 0)
    lane = lax.broadcasted_iota(jnp.int32, (8, 128), 1)
    parts = []
    for g in range(GROUPS):
        z = zb[g]
        loss = jnp.maximum(z, 0.0) + jnp.log1p(jnp.exp(-jnp.abs(z))) - yb[...] * z
        rows = pl.ds(0, R)
        sq = w1[g, rows, :] * w1[g, rows, :] / PRIOR_VAR + p1[g, rows, :] * p1[g, rows, :]
        sqo = w2[g, rows, :] * w2[g, rows, :] / PRIOR_VAR + p2[g, rows, :] * p2[g, rows, :]
        sq = jnp.sum(sq.reshape(NT, 8, DP), axis=0)
        sqo = jnp.sum(sqo.reshape(NT, 8, 128), axis=0)
        quad = jnp.sum(sq, axis=1, keepdims=True) + sqo
        quad = quad + pltpu.roll(quad, 4, 0)
        parts.append(jnp.sum(loss, axis=1, keepdims=True) + 0.5 * quad)
    ener = jnp.where(sub < 4, parts[0], parts[1])
    ener = jnp.sum(jnp.where(sub == lane % 8, ener, 0.0), axis=0, keepdims=True)
    place_out(pack(p1, p2, packp), packp)
    packp[pl.ds(15 * 8, 8), pl.ds(64, 64)] = jnp.broadcast_to(ener[:, 0:64], (8, 64))
    state["p"] = send_pack(packp, recvp, sp, rp)

    lane1 = lax.broadcasted_iota(jnp.int32, (1, 128), 1)

    def unpack(q, slab, out3, out2):
        rows = pl.ds(pl.multiple_of(q * 8, 8), 8)
        for j in range(16):
            v = slab[pl.ds(j * 8, 8), :]
            out3[j, rows, :] = v[:, 0:H]
            if j + 16 < D:
                out3[j + 16, rows, :] = pltpu.roll(v, 64, 1)[:, 0:H]
            elif j + 16 == D:
                out2[rows, :] = pltpu.roll(v, 64, 1)[:, 0:H]

    def energy_of(q, slab, cur):
        v = pltpu.roll(slab[pl.ds(15 * 8, 8), :], 64, 1)[0:1, :]
        return jnp.where(lane1 // 8 == q, v, cur)

    unpack(me, packw, end_w, end_wo)
    unpack(me, packp, end_p, end_po)
    en = energy_of(me, packp, jnp.zeros((1, 128), f32))
    for c in state["w"]:
        c.wait()
    for k in (1, 2, 3):
        unpack(peers[k], recvw.at[k], end_w, end_wo)
    for c in state["p"]:
        c.wait()
    for k in (1, 2, 3):
        unpack(peers[k], recvp.at[k], end_p, end_po)
        en = energy_of(peers[k], recvp.at[k], en)
    end_e[...] = en[:, 0:32]


def store_kernel(*refs):
    sems = refs[-1]
    copies = [pltpu.make_async_copy(refs[i], refs[5 + i], sems.at[i]) for i in range(5)]
    for c in copies:
        c.start()
    for c in copies:
        c.wait()


def solution(mesh):
    row_spec = P('data', None)
    label_spec = P('data')
    in_spec = P(None, 'parts', None)
    out_spec = P('parts', None)
    chain_spec = P('parts')

    def run_chains(feats, labels, w_in, w_out, mom_in, mom_out):
        n_rows, D = feats.shape
        H = w_in.shape[2]
        eps = 1.0 / math.sqrt(n_rows * (D + H))

        def device_body(x_rows, y_rows, wi, wo, mi, mo):
            rows_dev = x_rows.shape[0]
            NT = 4 * H // 8
            R = NT * 8
            dims = (D, H, rows_dev, n_rows, eps, 0.5 * eps)
            S = jax.ShapeDtypeStruct
            hbm = pl.BlockSpec(memory_space=pltpu.HBM)
            vm = pl.BlockSpec(memory_space=pltpu.VMEM)
            V = pltpu.VMEM
            dma = pltpu.SemaphoreType.DMA
            out = pl.pallas_call(
                functools.partial(kernel, dims),
                name='hmc',
                out_shape=[S(wi.shape, f32), S(wo.shape, f32), S(wi.shape, f32), S(wo.shape, f32), S((1, wo.shape[0]), f32)],
                in_specs=[hbm] * 6,
                out_specs=[vm] * 5,
                scratch_shapes=[
                    V((D, rows_dev), bf16), V((rows_dev // 128, 128), jnp.int32),
                    V((D, 8, H), f32), V((D, 8, H), f32), V((8, H), f32), V((8, H), f32),
                    V((DP, rows_dev), bf16), V((4, DP, rows_dev), bf16), V((4, rows_dev // 128, 128), jnp.int32),
                    V((DP, n_rows), f32), V((8, n_rows), f32),
                    V((GROUPS, 4 * HP, DP), f32), V((GROUPS, 4 * HP, 128), f32), V((GROUPS, 4 * HP, DP), f32), V((GROUPS, 4 * HP, 128), f32),
                    V((GROUPS, 8, n_rows), f32),
                    V((4, R, CHUNK), f32), V((4, R, CHUNK), f32), V((4, R, CHUNK), f32), V((GROUPS, R, 128), f32),
                    V((LEAD, R, CHUNK), f32), V((R, DP), f32),
                    V((128, 128), f32), V((128, 128), f32), V((4, 128, 128), f32), V((4, 128, 128), f32),
                    dma((6,)), dma((4,)), dma((4,)), dma((4,)), dma((4,)), dma((4,)), dma((4,)), dma((4,)), dma((4,)),
                ],
                compiler_params=pltpu.CompilerParams(collective_id=0, has_side_effects=True, vmem_limit_bytes=48 * 1024 * 1024),
            )(*[pltpu.with_memory_space_constraint(a, pltpu.HBM) for a in (x_rows.T, y_rows.reshape(rows_dev // 128, 128), wi, wo, mi, mo)])
            out = pl.pallas_call(
                store_kernel,
                name='store',
                out_shape=[S(o.shape, o.dtype) for o in out],
                in_specs=[vm] * 5,
                out_specs=[hbm] * 5,
                scratch_shapes=[dma((5,))],
                compiler_params=pltpu.CompilerParams(vmem_limit_bytes=4 * 1024 * 1024),
            )(*out)
            return out[0], out[1], out[2], out[3], out[4].reshape(-1)

        mapped = jax.shard_map(device_body, mesh=mesh, in_specs=(row_spec, label_spec, in_spec, out_spec, in_spec, out_spec),
                               out_specs=(in_spec, out_spec, in_spec, out_spec, chain_spec), check_vma=False)
        return mapped(feats, labels, w_in, w_out, mom_in, mom_out)

    return run_chains
```

```python
import functools
import math

import jax
import jax.numpy as jnp
from jax import lax
from jax.experimental import pallas as pl
from jax.experimental.pallas import tpu as pltpu
from jax.sharding import PartitionSpec as P

LEAPS = 16
PRIOR_VAR = 1.0
MESH = pl.DeviceIdType.MESH
f32 = jnp.float32
bf16 = jnp.bfloat16

GROUPS = 2
CHUNK = 256
DP = 32
HP = 64
LEAD = 2
LAG = 2
UNROLL = 8


def cat2(x):
    return jnp.concatenate([x, x], axis=1)


def kernel(dims, feats, labels, w_in, w_out, mom_in, mom_out, end_w, end_wo, end_p, end_po, end_e,
           xs, ls, wsl, psl, wos, pos, xsend, xrecv, lrecv, xf, yb, w1, w2, p1, p2,
           zb, act, slope, bgr, accw, araw, gpart, packw, packp, recvw, recvp,
           in_sem, sx, rx, sl, rl, sw, rw, sp, rp):
    D, H, rows_dev, n_rows, eps, half = dims
    G4 = 4
    NT = G4 * H // 8
    R = NT * 8
    NC = n_rows // CHUNK
    U = GROUPS * NC
    me = lax.axis_index("data")
    xi = me // 2
    ci = me % 2
    peers = {1: xi * 2 + (1 - ci), 2: (1 - xi) * 2 + ci, 3: (1 - xi) * 2 + (1 - ci)}
    mine = pl.ds(pl.multiple_of(me * 8, 8), 8)

    copies = [
        pltpu.make_async_copy(feats, xs, in_sem.at[0]),
        pltpu.make_async_copy(labels, ls, in_sem.at[1]),
        pltpu.make_async_copy(w_in.at[:, mine, :], wsl, in_sem.at[2]),
        pltpu.make_async_copy(mom_in.at[:, mine, :], psl, in_sem.at[3]),
        pltpu.make_async_copy(w_out.at[mine, :], wos, in_sem.at[4]),
        pltpu.make_async_copy(mom_out.at[mine, :], pos, in_sem.at[5]),
    ]
    for c in copies:
        c.start()
    barrier = pltpu.get_barrier_semaphore()
    for k in peers:
        pl.semaphore_signal(barrier, inc=1, device_id={"data": peers[k]}, device_id_type=MESH)

    copies[0].wait()
    copies[1].wait()
    xf[:, pl.ds(0, rows_dev)] = jnp.zeros((DP, rows_dev), f32)
    xf[pl.ds(0, D), pl.ds(0, rows_dev)] = xs[...].astype(f32)
    xsend[...] = xf[:, pl.ds(0, rows_dev)].astype(bf16)
    pl.semaphore_wait(barrier, 3)
    sends = []
    for k in (2, 3, 1):
        sends.append(pltpu.make_async_remote_copy(src_ref=xsend, dst_ref=xrecv.at[k], send_sem=sx.at[k], recv_sem=rx.at[k],
                                                  device_id={"data": peers[k]}, device_id_type=MESH))
        sends.append(pltpu.make_async_remote_copy(src_ref=ls, dst_ref=lrecv.at[k], send_sem=sl.at[k], recv_sem=rl.at[k],
                                                  device_id={"data": peers[k]}, device_id_type=MESH))
    for s in sends:
        s.start()

    for c in copies[2:]:
        c.wait()
    for ref in (w1, p1):
        ref[...] = jnp.zeros_like(ref)
    for src, dst in ((wsl, w1), (psl, p1)):
        for c in range(8):
            dst[c // 4, pl.ds(c % 4, H, stride=4), pl.ds(0, D)] = src[:, c, :].T
    for src, dst in ((wos, w2), (pos, p2)):
        t = src[...].T
        for c in range(8):
            dst[c // 4, pl.ds(c % 4, H, stride=4), :] = jnp.broadcast_to(t[:, c:c + 1], (H, 128))
    for u in range(4 - LAG, 4):
        act[u] = jnp.zeros((R, CHUNK), f32)
        slope[u] = jnp.zeros((R, CHUNK), f32)
    accw[1] = jnp.zeros((R, 128), f32)
    gpart[...] = jnp.zeros((R, DP), f32)
    zb[...] = jnp.zeros_like(zb)

    def put_labels(k, lab):
        lab = lab.astype(f32)
        for j in range(rows_dev // 128):
            yb[:, pl.ds(k * rows_dev + j * 128, 128)] = jnp.broadcast_to(lab[j:j + 1, :], (8, 128))

    put_labels(0, ls[...])
    for s in sends:
        s.wait()
    for k in (1, 2, 3):
        xf[:, pl.ds(k * rows_dev, rows_dev)] = xrecv[k].astype(f32)
        put_labels(k, lrecv[k])

    def cols(u):
        return pl.ds((u % NC) * CHUNK, CHUNK)

    def grp(u):
        return (u % U) // NC

    def mm_act(u):
        return jnp.dot(w1[grp(u), pl.ds(0, R), :], xf[:, cols(u)], preferred_element_type=f32)

    def mm_grad(u):
        return lax.dot_general(bgr[u % 4], xf[:, cols(u)], (((1,), (1,)), ((), ())), preferred_element_type=f32)

    def resid(u):
        return yb[:, cols(u)] - jax.nn.sigmoid(zb[grp(u), :, cols(u)])

    def forward(u, pre):
        g, s = grp(u), u % 4
        z = None
        for h in range(NT):
            rows = pl.ds(h * 8, 8)
            wo = cat2(w2[g, rows, :])
            a = jnp.tanh(pre[h * 8:(h + 1) * 8, :])
            t = a * wo
            z = t if z is None else z + t
            act[s, rows, :] = a
            slope[s, rows, :] = wo - t * a
        zb[g, :, cols(u)] = z + pltpu.roll(z, 4, 0)

    def backward(u, r):
        g, s = grp(u), u % 4
        for h in range(NT):
            rows = pl.ds(h * 8, 8)
            ra = r * act[s, rows, :]
            ra = ra[:, :128] + ra[:, 128:]
            if u % NC == 0:
                accw[g, rows, :] = ra
            else:
                accw[g, rows, :] += ra
            bgr[u % 4, rows, :] = r * slope[s, rows, :]

    def update(g, grad, e, f):
        rows = pl.ds(0, R)
        w = w1[g, rows, :]
        p = p1[g, rows, :] + e * (grad - w / PRIOR_VAR)
        p1[g, rows, :] = p
        w1[g, rows, :] = w + f * p
        gw = jnp.sum(accw[g], axis=1, keepdims=True)
        w = w2[g, rows, :]
        p = p2[g, rows, :] + e * (gw - w / PRIOR_VAR)
        p2[g, rows, :] = p
        w2[g, rows, :] = w + f * p

    def slots(final, e_prev, f_prev, e_now, f_now, after1=None, after0=None):
        ahead = {}
        grad = None
        for s in range(U):
            if not (final and s + LEAD >= U):
                ahead[s + LEAD] = mm_act(s + LEAD)
            u = (s - LAG) % U
            r = resid(u)
            forward(s, araw[s] if s < LEAD else ahead.pop(s))
            backward(u, r)
            g = mm_grad(u)
            if s == 0:
                grad = gpart[...]
            grad = g if grad is None else grad + g
            if s == LAG - 1:
                update(1, grad, e_prev, f_prev)
                grad = None
                if after1 is not None:
                    after1()
            elif s == NC + LAG - 1:
                update(0, grad, e_now, f_now)
                grad = None
                if after0 is not None:
                    after0()
        return ahead, grad

    for k in range(LEAD):
        araw[k] = mm_act(k)

    def step(i, carry):
        e_prev = jnp.where(i == 0, 0.0, jnp.where(i == 1, half, eps))
        f_prev = jnp.where(i == 0, 0.0, eps)
        e_now = jnp.where(i == 0, half, eps)
        ahead, grad = slots(False, e_prev, f_prev, e_now, eps)
        for k in range(LEAD):
            araw[k] = ahead[U + k]
        gpart[...] = grad
        return carry

    lax.fori_loop(0, LEAPS, step, 0, unroll=UNROLL)

    sub = lax.broadcasted_iota(jnp.int32, (8, 128), 0)
    lane = lax.broadcasted_iota(jnp.int32, (8, 128), 1)
    lane_h = lax.broadcasted_iota(jnp.int32, (HP, 128), 1)

    def pack(g, src, src_o, dst):
        o = jnp.zeros((HP, 128), f32)
        for c in range(4):
            rows = pl.ds(c, HP, stride=4)
            t = src[g, rows, :].T
            dst[g, pl.ds(c, 16, stride=4), :] = jnp.concatenate([t[0:16], t[16:32]], axis=1)
            o = jnp.where(lane_h == c, src_o[g, rows, :], o)
        dst[g, pl.ds(48, 4), pl.ds(64, 64)] = o.T[0:4, :]

    def copy_to(peer, src, dst, ss, rs):
        return pltpu.make_async_remote_copy(src_ref=src, dst_ref=dst, send_sem=ss, recv_sem=rs,
                                            device_id={"data": peers[peer]}, device_id_type=MESH)

    def send(g, src, dst, ss, rs, to):
        out = {}
        for k in to:
            out[k] = copy_to(k, src.at[g], dst.at[k, g], ss.at[k, g], rs.at[k, g])
            out[k].start()
        return out

    def forward_on(g, dst, ss, rs):
        c = copy_to(1, dst.at[2, g], dst.at[3, g], ss.at[3, g], rs.at[3, g])
        c.start()
        return c

    def energy(g):
        z = zb[g]
        loss = jnp.maximum(z, 0.0) + jnp.log1p(jnp.exp(-jnp.abs(z))) - yb[...] * z
        rows = pl.ds(0, R)
        sq = w1[g, rows, :] * w1[g, rows, :] / PRIOR_VAR + p1[g, rows, :] * p1[g, rows, :]
        sqo = w2[g, rows, :] * w2[g, rows, :] / PRIOR_VAR + p2[g, rows, :] * p2[g, rows, :]
        sq = jnp.sum(sq.reshape(NT, 8, DP), axis=0)
        sqo = jnp.sum(sqo.reshape(NT, 8, 128), axis=0)
        quad = jnp.sum(sq, axis=1, keepdims=True) + sqo
        quad = quad + pltpu.roll(quad, 4, 0)
        return jnp.sum(loss, axis=1, keepdims=True) + 0.5 * quad

    def send_momenta(g, to):
        packp[g, pl.ds(56, 4), pl.ds(64, 64)] = energy(g)[0:4, 0:64]
        return send(g, packp, recvp, sp, rp, to)

    sent = {}

    def send_w0():
        pack(0, w1, w2, packw)
        sent["w0"] = send(0, packw, recvw, sw, rw, (2, 1))

    def send_w1():
        pack(1, w1, w2, packw)
        sent["w1"] = send(1, packw, recvw, sw, rw, (2, 1))

    def send_p0():
        pack(0, p1, p2, packp)
        sent["p0"] = send_momenta(0, (2, 1))

    send_w0()
    ahead, grad = slots(True, eps, eps, half, 0.0, send_w1, send_p0)
    for u in range(U - LAG, U):
        backward(u, resid(u))
        grad = grad + mm_grad(u)
    update(1, grad, half, 0.0)
    pack(1, p1, p2, packp)
    sent["p1"] = send_momenta(1, (2, 3, 1))

    lane1 = lax.broadcasted_iota(jnp.int32, (1, 128), 1)

    def unpack(q, bufs, out3, out2, en):
        rows = pl.ds(pl.multiple_of(q * 8, 8), 8)
        for j in range(8):
            b0 = bufs[0, pl.ds(j * 8, 8), :]
            b1 = bufs[1, pl.ds(j * 8, 8), :]
            for r, v in ((2 * j, jnp.where(sub < 4, b0, pltpu.roll(b1, 4, 0))),
                         (2 * j + 1, jnp.where(sub < 4, pltpu.roll(b0, 4, 0), b1))):
                out3[r, rows, :] = v[:, 0:H]
                if r <= 12 or r == 14:
                    t = pltpu.roll(v, 64, 1)
                    if r < 12:
                        out3[r + 16, rows, :] = t[:, 0:H]
                    elif r == 12:
                        out2[rows, :] = t[:, 0:H]
                    elif en is not None:
                        t = jnp.sum(jnp.where(sub == lane % 8, t, 0.0), axis=0, keepdims=True)
                        en = jnp.where(lane1 // 8 == q, t, en)
        return en

    for name, g in (("w0", 0), ("w1", 1)):
        sent[name][2].wait()
        sent[name][3] = forward_on(g, recvw, sw, rw)
    unpack(me, packw, end_w, end_wo, None)
    en = unpack(me, packp, end_p, end_po, jnp.zeros((1, 128), f32))
    sent["p0"][2].wait()
    sent["p0"][3] = forward_on(0, recvp, sp, rp)
    for k in (1, 2, 3):
        for name in ("w0", "w1"):
            if k != 2:
                sent[name][k].wait()
        unpack(peers[k], recvw.at[k], end_w, end_wo, None)
    for k in (1, 2, 3):
        if k != 2:
            sent["p0"][k].wait()
        sent["p1"][k].wait()
        en = unpack(peers[k], recvp.at[k], end_p, end_po, en)
    end_e[...] = en[:, 0:32]


def store_kernel(*refs):
    sems = refs[-1]
    copies = [pltpu.make_async_copy(refs[i], refs[5 + i], sems.at[i]) for i in range(5)]
    for c in copies:
        c.start()
    for c in copies:
        c.wait()


def solution(mesh):
    row_spec = P('data', None)
    label_spec = P('data')
    in_spec = P(None, 'parts', None)
    out_spec = P('parts', None)
    chain_spec = P('parts')

    def run_chains(feats, labels, w_in, w_out, mom_in, mom_out):
        n_rows, D = feats.shape
        H = w_in.shape[2]
        eps = 1.0 / math.sqrt(n_rows * (D + H))

        def device_body(x_rows, y_rows, wi, wo, mi, mo):
            rows_dev = x_rows.shape[0]
            NT = 4 * H // 8
            R = NT * 8
            dims = (D, H, rows_dev, n_rows, eps, 0.5 * eps)
            S = jax.ShapeDtypeStruct
            hbm = pl.BlockSpec(memory_space=pltpu.HBM)
            vm = pl.BlockSpec(memory_space=pltpu.VMEM)
            V = pltpu.VMEM
            dma = pltpu.SemaphoreType.DMA
            out = pl.pallas_call(
                functools.partial(kernel, dims),
                name='hmc',
                out_shape=[S(wi.shape, f32), S(wo.shape, f32), S(wi.shape, f32), S(wo.shape, f32), S((1, wo.shape[0]), f32)],
                in_specs=[hbm] * 6,
                out_specs=[vm] * 5,
                scratch_shapes=[
                    V((D, rows_dev), bf16), V((rows_dev // 128, 128), jnp.int32),
                    V((D, 8, H), f32), V((D, 8, H), f32), V((8, H), f32), V((8, H), f32),
                    V((DP, rows_dev), bf16), V((4, DP, rows_dev), bf16), V((4, rows_dev // 128, 128), jnp.int32),
                    V((DP, n_rows), f32), V((8, n_rows), f32),
                    V((GROUPS, 4 * HP, DP), f32), V((GROUPS, 4 * HP, 128), f32), V((GROUPS, 4 * HP, DP), f32), V((GROUPS, 4 * HP, 128), f32),
                    V((GROUPS, 8, n_rows), f32),
                    V((4, R, CHUNK), f32), V((4, R, CHUNK), f32), V((4, R, CHUNK), f32), V((GROUPS, R, 128), f32),
                    V((LEAD, R, CHUNK), f32), V((R, DP), f32),
                    V((2, 64, 128), f32), V((2, 64, 128), f32), V((4, 2, 64, 128), f32), V((4, 2, 64, 128), f32),
                    dma((6,)), dma((4,)), dma((4,)), dma((4,)), dma((4,)), dma((4, 2)), dma((4, 2)), dma((4, 2)), dma((4, 2)),
                ],
                compiler_params=pltpu.CompilerParams(collective_id=0, has_side_effects=True, vmem_limit_bytes=48 * 1024 * 1024),
            )(*[pltpu.with_memory_space_constraint(a, pltpu.HBM) for a in (x_rows.T, y_rows.reshape(rows_dev // 128, 128), wi, wo, mi, mo)])
            out = pl.pallas_call(
                store_kernel,
                name='store',
                out_shape=[S(o.shape, o.dtype) for o in out],
                in_specs=[vm] * 5,
                out_specs=[hbm] * 5,
                scratch_shapes=[dma((5,))],
                compiler_params=pltpu.CompilerParams(vmem_limit_bytes=4 * 1024 * 1024),
            )(*out)
            return out[0], out[1], out[2], out[3], out[4].reshape(-1)

        mapped = jax.shard_map(device_body, mesh=mesh, in_specs=(row_spec, label_spec, in_spec, out_spec, in_spec, out_spec),
                               out_specs=(in_spec, out_spec, in_spec, out_spec, chain_spec), check_vma=False)
        return mapped(feats, labels, w_in, w_out, mom_in, mom_out)

    return run_chains
```

```python
import functools
import math

import jax
import jax.numpy as jnp
from jax import lax
from jax.experimental import pallas as pl
from jax.experimental.pallas import tpu as pltpu
from jax.sharding import PartitionSpec as P

LEAPS = 16
PRIOR_VAR = 1.0
MESH = pl.DeviceIdType.MESH
f32 = jnp.float32
bf16 = jnp.bfloat16

GROUPS = 2
CHUNK = 256
DP = 32
HP = 64
LEAD = 2
LAG = 2
UNROLL = 8


def cat2(x):
    return jnp.concatenate([x, x], axis=1)


def kernel(dims, feats, labels, w_in, w_out, mom_in, mom_out, end_w, end_wo, end_p, end_po, end_e,
           xs, ls, wsl, psl, wos, pos, xsend, xrecv, lrecv, xf, yb, w1, w2, p1, p2,
           zb, act, slope, bgr, accw, araw, gpart, packw, packp, recvw, recvp,
           in_sem, sx, rx, sl, rl, sw, rw, sp, rp):
    D, H, rows_dev, n_rows, eps, half = dims
    G4 = 4
    NT = G4 * H // 8
    R = NT * 8
    NC = n_rows // CHUNK
    U = GROUPS * NC
    me = lax.axis_index("data")
    xi = me // 2
    ci = me % 2
    peers = {1: xi * 2 + (1 - ci), 2: (1 - xi) * 2 + ci, 3: (1 - xi) * 2 + (1 - ci)}
    mine = pl.ds(pl.multiple_of(me * 8, 8), 8)

    copies = [
        pltpu.make_async_copy(feats, xs, in_sem.at[0]),
        pltpu.make_async_copy(labels, ls, in_sem.at[1]),
        pltpu.make_async_copy(w_in.at[:, mine, :], wsl, in_sem.at[2]),
        pltpu.make_async_copy(mom_in.at[:, mine, :], psl, in_sem.at[3]),
        pltpu.make_async_copy(w_out.at[mine, :], wos, in_sem.at[4]),
        pltpu.make_async_copy(mom_out.at[mine, :], pos, in_sem.at[5]),
    ]
    for c in copies:
        c.start()
    barrier = pltpu.get_barrier_semaphore()
    for k in peers:
        pl.semaphore_signal(barrier, inc=1, device_id={"data": peers[k]}, device_id_type=MESH)

    copies[0].wait()
    copies[1].wait()
    xf[:, pl.ds(0, rows_dev)] = jnp.zeros((DP, rows_dev), f32)
    xf[pl.ds(0, D), pl.ds(0, rows_dev)] = xs[...].astype(f32)
    xsend[...] = xf[:, pl.ds(0, rows_dev)].astype(bf16)
    pl.semaphore_wait(barrier, 3)
    sends = []
    for k in (2, 3, 1):
        sends.append(pltpu.make_async_remote_copy(src_ref=xsend, dst_ref=xrecv.at[k], send_sem=sx.at[k], recv_sem=rx.at[k],
                                                  device_id={"data": peers[k]}, device_id_type=MESH))
        sends.append(pltpu.make_async_remote_copy(src_ref=ls, dst_ref=lrecv.at[k], send_sem=sl.at[k], recv_sem=rl.at[k],
                                                  device_id={"data": peers[k]}, device_id_type=MESH))
    for s in sends:
        s.start()

    for c in copies[2:]:
        c.wait()
    for ref in (w1, p1):
        ref[...] = jnp.zeros_like(ref)
    for src, dst in ((wsl, w1), (psl, p1)):
        for c in range(8):
            dst[c // 4, pl.ds(c % 4, H, stride=4), pl.ds(0, D)] = src[:, c, :].T
    for src, dst in ((wos, w2), (pos, p2)):
        t = src[...].T
        for c in range(8):
            dst[c // 4, pl.ds(c % 4, H, stride=4), :] = jnp.broadcast_to(t[:, c:c + 1], (H, 128))
    for u in range(4 - LAG, 4):
        act[u] = jnp.zeros((R, CHUNK), f32)
        slope[u] = jnp.zeros((R, CHUNK), f32)
    accw[1] = jnp.zeros((R, 128), f32)
    gpart[...] = jnp.zeros((R, DP), f32)
    zb[...] = jnp.zeros_like(zb)

    def put_labels(k, lab):
        lab = lab.astype(f32)
        for j in range(rows_dev // 128):
            yb[:, pl.ds(k * rows_dev + j * 128, 128)] = jnp.broadcast_to(lab[j:j + 1, :], (8, 128))

    put_labels(0, ls[...])
    def cols(u):
        return pl.ds((u % NC) * CHUNK, CHUNK)

    def grp(u):
        return (u % U) // NC

    def mm_act(u):
        return jnp.dot(w1[grp(u), pl.ds(0, R), :], xf[:, cols(u)], preferred_element_type=f32)

    def mm_grad(u):
        return lax.dot_general(bgr[u % 4], xf[:, cols(u)], (((1,), (1,)), ((), ())), preferred_element_type=f32)

    def resid(u):
        return yb[:, cols(u)] - jax.nn.sigmoid(zb[grp(u), :, cols(u)])

    def forward(u, pre):
        g, s = grp(u), u % 4
        z = None
        for h in range(NT):
            rows = pl.ds(h * 8, 8)
            wo = cat2(w2[g, rows, :])
            a = jnp.tanh(pre[h * 8:(h + 1) * 8, :])
            t = a * wo
            z = t if z is None else z + t
            act[s, rows, :] = a
            slope[s, rows, :] = wo - t * a
        zb[g, :, cols(u)] = z + pltpu.roll(z, 4, 0)

    def backward(u, r):
        g, s = grp(u), u % 4
        for h in range(NT):
            rows = pl.ds(h * 8, 8)
            ra = r * act[s, rows, :]
            ra = ra[:, :128] + ra[:, 128:]
            if u % NC == 0:
                accw[g, rows, :] = ra
            else:
                accw[g, rows, :] += ra
            bgr[u % 4, rows, :] = r * slope[s, rows, :]

    def update(g, grad, e, f):
        rows = pl.ds(0, R)
        w = w1[g, rows, :]
        p = p1[g, rows, :] + e * (grad - w / PRIOR_VAR)
        p1[g, rows, :] = p
        w1[g, rows, :] = w + f * p
        gw = jnp.sum(accw[g], axis=1, keepdims=True)
        w = w2[g, rows, :]
        p = p2[g, rows, :] + e * (gw - w / PRIOR_VAR)
        p2[g, rows, :] = p
        w2[g, rows, :] = w + f * p

    def slots(final, e_prev, f_prev, e_now, f_now, after1=None, after0=None):
        ahead = {}
        grad = None
        for s in range(U):
            if not (final and s + LEAD >= U):
                ahead[s + LEAD] = mm_act(s + LEAD)
            u = (s - LAG) % U
            r = resid(u)
            forward(s, araw[s] if s < LEAD else ahead.pop(s))
            backward(u, r)
            g = mm_grad(u)
            if s == 0:
                grad = gpart[...]
            grad = g if grad is None else grad + g
            if s == LAG - 1:
                update(1, grad, e_prev, f_prev)
                grad = None
                if after1 is not None:
                    after1()
            elif s == NC + LAG - 1:
                update(0, grad, e_now, f_now)
                grad = None
                if after0 is not None:
                    after0()
        return ahead, grad

    for k in range(LEAD):
        araw[k] = mm_act(k)
    for s in sends:
        s.wait()
    for k in (1, 2, 3):
        xf[:, pl.ds(k * rows_dev, rows_dev)] = xrecv[k].astype(f32)
        put_labels(k, lrecv[k])

    def step(i, carry):
        e_prev = jnp.where(i == 0, 0.0, jnp.where(i == 1, half, eps))
        f_prev = jnp.where(i == 0, 0.0, eps)
        e_now = jnp.where(i == 0, half, eps)
        ahead, grad = slots(False, e_prev, f_prev, e_now, eps)
        for k in range(LEAD):
            araw[k] = ahead[U + k]
        gpart[...] = grad
        return carry

    lax.fori_loop(0, LEAPS, step, 0, unroll=UNROLL)

    sub = lax.broadcasted_iota(jnp.int32, (8, 128), 0)
    lane = lax.broadcasted_iota(jnp.int32, (8, 128), 1)
    lane_h = lax.broadcasted_iota(jnp.int32, (HP, 128), 1)

    def pack(g, src, src_o, dst):
        o = jnp.zeros((HP, 128), f32)
        for c in range(4):
            rows = pl.ds(c, HP, stride=4)
            t = src[g, rows, :].T
            dst[g, pl.ds(c, 16, stride=4), :] = jnp.concatenate([t[0:16], t[16:32]], axis=1)
            o = jnp.where(lane_h == c, src_o[g, rows, :], o)
        dst[g, pl.ds(48, 4), pl.ds(64, 64)] = o.T[0:4, :]

    def copy_to(peer, src, dst, ss, rs):
        return pltpu.make_async_remote_copy(src_ref=src, dst_ref=dst, send_sem=ss, recv_sem=rs,
                                            device_id={"data": peers[peer]}, device_id_type=MESH)

    def send(g, src, dst, ss, rs, to):
        out = {}
        for k in to:
            out[k] = copy_to(k, src.at[g], dst.at[k, g], ss.at[k, g], rs.at[k, g])
            out[k].start()
        return out

    def forward_on(g, dst, ss, rs):
        c = copy_to(1, dst.at[2, g], dst.at[3, g], ss.at[3, g], rs.at[3, g])
        c.start()
        return c

    def energy(g):
        z = zb[g]
        loss = jnp.maximum(z, 0.0) + jnp.log1p(jnp.exp(-jnp.abs(z))) - yb[...] * z
        rows = pl.ds(0, R)
        sq = w1[g, rows, :] * w1[g, rows, :] / PRIOR_VAR + p1[g, rows, :] * p1[g, rows, :]
        sqo = w2[g, rows, :] * w2[g, rows, :] / PRIOR_VAR + p2[g, rows, :] * p2[g, rows, :]
        sq = jnp.sum(sq.reshape(NT, 8, DP), axis=0)
        sqo = jnp.sum(sqo.reshape(NT, 8, 128), axis=0)
        quad = jnp.sum(sq, axis=1, keepdims=True) + sqo
        quad = quad + pltpu.roll(quad, 4, 0)
        return jnp.sum(loss, axis=1, keepdims=True) + 0.5 * quad

    def send_momenta(g, to):
        packp[g, pl.ds(56, 4), pl.ds(64, 64)] = energy(g)[0:4, 0:64]
        return send(g, packp, recvp, sp, rp, to)

    sent = {}

    def send_w0():
        pack(0, w1, w2, packw)
        sent["w0"] = send(0, packw, recvw, sw, rw, (2, 1))

    def send_w1():
        pack(1, w1, w2, packw)
        sent["w1"] = send(1, packw, recvw, sw, rw, (2, 1))

    def send_p0():
        pack(0, p1, p2, packp)
        sent["p0"] = send_momenta(0, (2, 1))

    send_w0()
    ahead, grad = slots(True, eps, eps, half, 0.0, send_w1, send_p0)
    for u in range(U - LAG, U):
        backward(u, resid(u))
        grad = grad + mm_grad(u)
    update(1, grad, half, 0.0)
    pack(1, p1, p2, packp)
    sent["p1"] = send_momenta(1, (2, 3, 1))

    lane1 = lax.broadcasted_iota(jnp.int32, (1, 128), 1)

    def unpack(q, bufs, out3, out2, en):
        rows = pl.ds(pl.multiple_of(q * 8, 8), 8)
        for j in range(8):
            b0 = bufs[0, pl.ds(j * 8, 8), :]
            b1 = bufs[1, pl.ds(j * 8, 8), :]
            for r, v in ((2 * j, jnp.where(sub < 4, b0, pltpu.roll(b1, 4, 0))),
                         (2 * j + 1, jnp.where(sub < 4, pltpu.roll(b0, 4, 0), b1))):
                out3[r, rows, :] = v[:, 0:H]
                if r <= 12 or r == 14:
                    t = pltpu.roll(v, 64, 1)
                    if r < 12:
                        out3[r + 16, rows, :] = t[:, 0:H]
                    elif r == 12:
                        out2[rows, :] = t[:, 0:H]
                    elif en is not None:
                        t = jnp.sum(jnp.where(sub == lane % 8, t, 0.0), axis=0, keepdims=True)
                        en = jnp.where(lane1 // 8 == q, t, en)
        return en

    for name, g in (("w0", 0), ("w1", 1)):
        sent[name][2].wait()
        sent[name][3] = forward_on(g, recvw, sw, rw)
    unpack(me, packw, end_w, end_wo, None)
    en = unpack(me, packp, end_p, end_po, jnp.zeros((1, 128), f32))
    sent["p0"][2].wait()
    sent["p0"][3] = forward_on(0, recvp, sp, rp)
    for k in (1, 2, 3):
        for name in ("w0", "w1"):
            if k != 2:
                sent[name][k].wait()
        unpack(peers[k], recvw.at[k], end_w, end_wo, None)
    for k in (1, 2, 3):
        if k != 2:
            sent["p0"][k].wait()
        sent["p1"][k].wait()
        en = unpack(peers[k], recvp.at[k], end_p, end_po, en)
    end_e[...] = en[:, 0:32]


def store_kernel(*refs):
    sems = refs[-1]
    copies = [pltpu.make_async_copy(refs[i], refs[5 + i], sems.at[i]) for i in range(5)]
    for c in copies:
        c.start()
    for c in copies:
        c.wait()


def solution(mesh):
    row_spec = P('data', None)
    label_spec = P('data')
    in_spec = P(None, 'parts', None)
    out_spec = P('parts', None)
    chain_spec = P('parts')

    def run_chains(feats, labels, w_in, w_out, mom_in, mom_out):
        n_rows, D = feats.shape
        H = w_in.shape[2]
        eps = 1.0 / math.sqrt(n_rows * (D + H))

        def device_body(x_rows, y_rows, wi, wo, mi, mo):
            rows_dev = x_rows.shape[0]
            NT = 4 * H // 8
            R = NT * 8
            dims = (D, H, rows_dev, n_rows, eps, 0.5 * eps)
            S = jax.ShapeDtypeStruct
            hbm = pl.BlockSpec(memory_space=pltpu.HBM)
            vm = pl.BlockSpec(memory_space=pltpu.VMEM)
            V = pltpu.VMEM
            dma = pltpu.SemaphoreType.DMA
            out = pl.pallas_call(
                functools.partial(kernel, dims),
                name='hmc',
                out_shape=[S(wi.shape, f32), S(wo.shape, f32), S(wi.shape, f32), S(wo.shape, f32), S((1, wo.shape[0]), f32)],
                in_specs=[hbm] * 6,
                out_specs=[vm] * 5,
                scratch_shapes=[
                    V((D, rows_dev), bf16), V((rows_dev // 128, 128), jnp.int32),
                    V((D, 8, H), f32), V((D, 8, H), f32), V((8, H), f32), V((8, H), f32),
                    V((DP, rows_dev), bf16), V((4, DP, rows_dev), bf16), V((4, rows_dev // 128, 128), jnp.int32),
                    V((DP, n_rows), f32), V((8, n_rows), f32),
                    V((GROUPS, 4 * HP, DP), f32), V((GROUPS, 4 * HP, 128), f32), V((GROUPS, 4 * HP, DP), f32), V((GROUPS, 4 * HP, 128), f32),
                    V((GROUPS, 8, n_rows), f32),
                    V((4, R, CHUNK), f32), V((4, R, CHUNK), f32), V((4, R, CHUNK), f32), V((GROUPS, R, 128), f32),
                    V((LEAD, R, CHUNK), f32), V((R, DP), f32),
                    V((2, 64, 128), f32), V((2, 64, 128), f32), V((4, 2, 64, 128), f32), V((4, 2, 64, 128), f32),
                    dma((6,)), dma((4,)), dma((4,)), dma((4,)), dma((4,)), dma((4, 2)), dma((4, 2)), dma((4, 2)), dma((4, 2)),
                ],
                compiler_params=pltpu.CompilerParams(collective_id=0, has_side_effects=True, vmem_limit_bytes=48 * 1024 * 1024),
            )(*[pltpu.with_memory_space_constraint(a, pltpu.HBM) for a in (x_rows.T, y_rows.reshape(rows_dev // 128, 128), wi, wo, mi, mo)])
            out = pl.pallas_call(
                store_kernel,
                name='store',
                out_shape=[S(o.shape, o.dtype) for o in out],
                in_specs=[vm] * 5,
                out_specs=[hbm] * 5,
                scratch_shapes=[dma((5,))],
                compiler_params=pltpu.CompilerParams(vmem_limit_bytes=4 * 1024 * 1024),
            )(*out)
            return out[0], out[1], out[2], out[3], out[4].reshape(-1)

        mapped = jax.shard_map(device_body, mesh=mesh, in_specs=(row_spec, label_spec, in_spec, out_spec, in_spec, out_spec),
                               out_specs=(in_spec, out_spec, in_spec, out_spec, chain_spec), check_vma=False)
        return mapped(feats, labels, w_in, w_out, mom_in, mom_out)

    return run_chains
```

```python
import functools
import math

import jax
import jax.numpy as jnp
from jax import lax
from jax.experimental import pallas as pl
from jax.experimental.pallas import tpu as pltpu
from jax.sharding import PartitionSpec as P

LEAPS = 16
PRIOR_VAR = 1.0
MESH = pl.DeviceIdType.MESH
f32 = jnp.float32
bf16 = jnp.bfloat16

GROUPS = 2
CHUNK = 256
DP = 32
HP = 64
LEAD = 2
LAG = 2
UNROLL = 8


def cat2(x):
    return jnp.concatenate([x, x], axis=1)


def kernel(dims, feats, labels, w_in, w_out, mom_in, mom_out, end_w, end_wo, end_p, end_po, end_e,
           xs, ls, wsl, psl, wos, pos, xsend, xrecv, lrecv, xf, yb, w1, w2, p1, p2,
           zb, act, slope, bgr, accw, araw, gpart, packw, packp, recvw, recvp,
           in_sem, sx, rx, sl, rl, sw, rw, sp, rp):
    D, H, rows_dev, n_rows, eps, half = dims
    G4 = 4
    NT = G4 * H // 8
    R = NT * 8
    NC = n_rows // CHUNK
    U = GROUPS * NC
    me = lax.axis_index("data")
    xi = me // 2
    ci = me % 2
    peers = {1: xi * 2 + (1 - ci), 2: (1 - xi) * 2 + ci, 3: (1 - xi) * 2 + (1 - ci)}
    mine = pl.ds(pl.multiple_of(me * 8, 8), 8)

    copies = [
        pltpu.make_async_copy(feats, xs, in_sem.at[0]),
        pltpu.make_async_copy(labels, ls, in_sem.at[1]),
        pltpu.make_async_copy(w_in.at[:, mine, :], wsl, in_sem.at[2]),
        pltpu.make_async_copy(mom_in.at[:, mine, :], psl, in_sem.at[3]),
        pltpu.make_async_copy(w_out.at[mine, :], wos, in_sem.at[4]),
        pltpu.make_async_copy(mom_out.at[mine, :], pos, in_sem.at[5]),
    ]
    for c in copies:
        c.start()
    barrier = pltpu.get_barrier_semaphore()
    for k in peers:
        pl.semaphore_signal(barrier, inc=1, device_id={"data": peers[k]}, device_id_type=MESH)

    copies[0].wait()
    copies[1].wait()
    xf[:, pl.ds(0, rows_dev)] = jnp.zeros((DP, rows_dev), f32)
    xf[pl.ds(0, D), pl.ds(0, rows_dev)] = xs[...].astype(f32)
    xsend[...] = xf[:, pl.ds(0, rows_dev)].astype(bf16)
    pl.semaphore_wait(barrier, 3)
    sends = []
    for k in (2, 3, 1):
        sends.append(pltpu.make_async_remote_copy(src_ref=xsend, dst_ref=xrecv.at[k], send_sem=sx.at[k], recv_sem=rx.at[k],
                                                  device_id={"data": peers[k]}, device_id_type=MESH))
        sends.append(pltpu.make_async_remote_copy(src_ref=ls, dst_ref=lrecv.at[k], send_sem=sl.at[k], recv_sem=rl.at[k],
                                                  device_id={"data": peers[k]}, device_id_type=MESH))
    for s in sends:
        s.start()

    for c in copies[2:]:
        c.wait()
    for ref in (w1, p1):
        ref[...] = jnp.zeros_like(ref)
    for src, dst in ((wsl, w1), (psl, p1)):
        for c in range(8):
            dst[c // 4, pl.ds(c % 4, H, stride=4), pl.ds(0, D)] = src[:, c, :].T
    for src, dst in ((wos, w2), (pos, p2)):
        t = src[...].T
        for c in range(8):
            dst[c // 4, pl.ds(c % 4, H, stride=4), :] = jnp.broadcast_to(t[:, c:c + 1], (H, 128))
    for u in range(4 - LAG, 4):
        act[u] = jnp.zeros((R, CHUNK), f32)
        slope[u] = jnp.zeros((R, CHUNK), f32)
    accw[1] = jnp.zeros((R, 128), f32)
    gpart[...] = jnp.zeros((R, DP), f32)
    zb[...] = jnp.zeros_like(zb)

    def put_labels(k, lab):
        lab = lab.astype(f32)
        for j in range(rows_dev // 128):
            yb[:, pl.ds(k * rows_dev + j * 128, 128)] = jnp.broadcast_to(lab[j:j + 1, :], (8, 128))

    put_labels(0, ls[...])
    def cols(u):
        return pl.ds((u % NC) * CHUNK, CHUNK)

    def grp(u):
        return (u % U) // NC

    def mm_act(u):
        return jnp.dot(w1[grp(u), pl.ds(0, R), :], xf[:, cols(u)], preferred_element_type=f32)

    def mm_grad(u):
        return lax.dot_general(bgr[u % 4], xf[:, cols(u)], (((1,), (1,)), ((), ())), preferred_element_type=f32)

    def resid(u):
        return yb[:, cols(u)] - jax.nn.sigmoid(zb[grp(u), :, cols(u)])

    def forward(u, pre):
        g, s = grp(u), u % 4
        z = None
        for h in range(NT):
            rows = pl.ds(h * 8, 8)
            wo = cat2(w2[g, rows, :])
            a = jnp.tanh(pre[h * 8:(h + 1) * 8, :])
            t = a * wo
            z = t if z is None else z + t
            act[s, rows, :] = a
            slope[s, rows, :] = wo - t * a
        zb[g, :, cols(u)] = z + pltpu.roll(z, 4, 0)

    def backward(u, r):
        g, s = grp(u), u % 4
        for h in range(NT):
            rows = pl.ds(h * 8, 8)
            ra = r * act[s, rows, :]
            ra = ra[:, :128] + ra[:, 128:]
            if u % NC == 0:
                accw[g, rows, :] = ra
            else:
                accw[g, rows, :] += ra
            bgr[u % 4, rows, :] = r * slope[s, rows, :]

    def update(g, grad, e, f):
        rows = pl.ds(0, R)
        w = w1[g, rows, :]
        p = p1[g, rows, :] + e * (grad - w / PRIOR_VAR)
        p1[g, rows, :] = p
        w1[g, rows, :] = w + f * p
        gw = jnp.sum(accw[g], axis=1, keepdims=True)
        w = w2[g, rows, :]
        p = p2[g, rows, :] + e * (gw - w / PRIOR_VAR)
        p2[g, rows, :] = p
        w2[g, rows, :] = w + f * p

    def slots(final, e_prev, f_prev, e_now, f_now, hooks={}):
        ahead = {}
        grad = None
        for s in range(U):
            if not (final and s + LEAD >= U):
                ahead[s + LEAD] = mm_act(s + LEAD)
            u = (s - LAG) % U
            r = resid(u)
            forward(s, araw[s] if s < LEAD else ahead.pop(s))
            backward(u, r)
            g = mm_grad(u)
            if s == 0:
                grad = gpart[...]
            grad = g if grad is None else grad + g
            if s == LAG - 1:
                update(1, grad, e_prev, f_prev)
                grad = None
            elif s == NC + LAG - 1:
                update(0, grad, e_now, f_now)
                grad = None
            for hook in hooks.get(s, ()):
                hook()
        return ahead, grad

    for k in range(LEAD):
        araw[k] = mm_act(k)
    for s in sends:
        s.wait()
    for k in (1, 2, 3):
        xf[:, pl.ds(k * rows_dev, rows_dev)] = xrecv[k].astype(f32)
        put_labels(k, lrecv[k])

    def step(i, carry):
        e_prev = jnp.where(i == 0, 0.0, jnp.where(i == 1, half, eps))
        f_prev = jnp.where(i == 0, 0.0, eps)
        e_now = jnp.where(i == 0, half, eps)
        ahead, grad = slots(False, e_prev, f_prev, e_now, eps)
        for k in range(LEAD):
            araw[k] = ahead[U + k]
        gpart[...] = grad
        return carry

    lax.fori_loop(0, LEAPS, step, 0, unroll=UNROLL)

    sub = lax.broadcasted_iota(jnp.int32, (8, 128), 0)
    lane = lax.broadcasted_iota(jnp.int32, (8, 128), 1)
    lane_h = lax.broadcasted_iota(jnp.int32, (HP, 128), 1)

    def pack(g, src, src_o, dst):
        o = jnp.zeros((HP, 128), f32)
        for c in range(4):
            rows = pl.ds(c, HP, stride=4)
            t = src[g, rows, :].T
            dst[g, pl.ds(c, 16, stride=4), :] = jnp.concatenate([t[0:16], t[16:32]], axis=1)
            o = jnp.where(lane_h == c, src_o[g, rows, :], o)
        dst[g, pl.ds(48, 4), pl.ds(64, 64)] = o.T[0:4, :]

    def copy_to(peer, src, dst, ss, rs):
        return pltpu.make_async_remote_copy(src_ref=src, dst_ref=dst, send_sem=ss, recv_sem=rs,
                                            device_id={"data": peers[peer]}, device_id_type=MESH)

    def send(g, src, dst, ss, rs, to):
        out = {}
        for k in to:
            out[k] = copy_to(k, src.at[g], dst.at[k, g], ss.at[k, g], rs.at[k, g])
            out[k].start()
        return out

    def forward_on(g, dst, ss, rs):
        c = copy_to(1, dst.at[2, g], dst.at[3, g], ss.at[3, g], rs.at[3, g])
        c.start()
        return c

    def energy(g):
        z = zb[g]
        loss = jnp.maximum(z, 0.0) + jnp.log1p(jnp.exp(-jnp.abs(z))) - yb[...] * z
        rows = pl.ds(0, R)
        sq = w1[g, rows, :] * w1[g, rows, :] / PRIOR_VAR + p1[g, rows, :] * p1[g, rows, :]
        sqo = w2[g, rows, :] * w2[g, rows, :] / PRIOR_VAR + p2[g, rows, :] * p2[g, rows, :]
        sq = jnp.sum(sq.reshape(NT, 8, DP), axis=0)
        sqo = jnp.sum(sqo.reshape(NT, 8, 128), axis=0)
        quad = jnp.sum(sq, axis=1, keepdims=True) + sqo
        quad = quad + pltpu.roll(quad, 4, 0)
        return jnp.sum(loss, axis=1, keepdims=True) + 0.5 * quad

    def pack_momenta(g):
        pack(g, p1, p2, packp)
        packp[g, pl.ds(56, 4), pl.ds(64, 64)] = energy(g)[0:4, 0:64]

    sent = {}

    def send_w0():
        pack(0, w1, w2, packw)
        sent["w0"] = send(0, packw, recvw, sw, rw, (2, 1))

    def pack_w1():
        pack(1, w1, w2, packw)

    def send_w1():
        sent["w1"] = send(1, packw, recvw, sw, rw, (2, 1))

    def pack_p0():
        pack_momenta(0)

    def send_p0():
        sent["p0"] = send(0, packp, recvp, sp, rp, (2, 1))

    send_w0()
    ahead, grad = slots(True, eps, eps, half, 0.0,
                        {LAG - 1: (pack_w1,), LAG + 2: (send_w1,), NC + LAG - 1: (pack_p0,), U - 2: (send_p0,)})
    for u in range(U - LAG, U):
        backward(u, resid(u))
        grad = grad + mm_grad(u)
    update(1, grad, half, 0.0)
    pack_momenta(1)
    sent["p1"] = send(1, packp, recvp, sp, rp, (2, 3, 1))

    lane1 = lax.broadcasted_iota(jnp.int32, (1, 128), 1)

    def unpack(q, bufs, out3, out2, en):
        rows = pl.ds(pl.multiple_of(q * 8, 8), 8)
        for j in range(8):
            b0 = bufs[0, pl.ds(j * 8, 8), :]
            b1 = bufs[1, pl.ds(j * 8, 8), :]
            for r, v in ((2 * j, jnp.where(sub < 4, b0, pltpu.roll(b1, 4, 0))),
                         (2 * j + 1, jnp.where(sub < 4, pltpu.roll(b0, 4, 0), b1))):
                out3[r, rows, :] = v[:, 0:H]
                if r <= 12 or r == 14:
                    t = pltpu.roll(v, 64, 1)
                    if r < 12:
                        out3[r + 16, rows, :] = t[:, 0:H]
                    elif r == 12:
                        out2[rows, :] = t[:, 0:H]
                    elif en is not None:
                        t = jnp.sum(jnp.where(sub == lane % 8, t, 0.0), axis=0, keepdims=True)
                        en = jnp.where(lane1 // 8 == q, t, en)
        return en

    for name, g in (("w0", 0), ("w1", 1)):
        sent[name][2].wait()
        sent[name][3] = forward_on(g, recvw, sw, rw)
    unpack(me, packw, end_w, end_wo, None)
    en = unpack(me, packp, end_p, end_po, jnp.zeros((1, 128), f32))
    sent["p0"][2].wait()
    sent["p0"][3] = forward_on(0, recvp, sp, rp)
    for k in (1, 2, 3):
        for name in ("w0", "w1"):
            if k != 2:
                sent[name][k].wait()
        unpack(peers[k], recvw.at[k], end_w, end_wo, None)
    for k in (1, 2, 3):
        if k != 2:
            sent["p0"][k].wait()
        sent["p1"][k].wait()
        en = unpack(peers[k], recvp.at[k], end_p, end_po, en)
    end_e[...] = en[:, 0:32]


def store_kernel(*refs):
    sems = refs[-1]
    copies = [pltpu.make_async_copy(refs[i], refs[5 + i], sems.at[i]) for i in range(5)]
    for c in copies:
        c.start()
    for c in copies:
        c.wait()


def solution(mesh):
    row_spec = P('data', None)
    label_spec = P('data')
    in_spec = P(None, 'parts', None)
    out_spec = P('parts', None)
    chain_spec = P('parts')

    def run_chains(feats, labels, w_in, w_out, mom_in, mom_out):
        n_rows, D = feats.shape
        H = w_in.shape[2]
        eps = 1.0 / math.sqrt(n_rows * (D + H))

        def device_body(x_rows, y_rows, wi, wo, mi, mo):
            rows_dev = x_rows.shape[0]
            NT = 4 * H // 8
            R = NT * 8
            dims = (D, H, rows_dev, n_rows, eps, 0.5 * eps)
            S = jax.ShapeDtypeStruct
            hbm = pl.BlockSpec(memory_space=pltpu.HBM)
            vm = pl.BlockSpec(memory_space=pltpu.VMEM)
            V = pltpu.VMEM
            dma = pltpu.SemaphoreType.DMA
            out = pl.pallas_call(
                functools.partial(kernel, dims),
                name='hmc',
                out_shape=[S(wi.shape, f32), S(wo.shape, f32), S(wi.shape, f32), S(wo.shape, f32), S((1, wo.shape[0]), f32)],
                in_specs=[hbm] * 6,
                out_specs=[vm] * 5,
                scratch_shapes=[
                    V((D, rows_dev), bf16), V((rows_dev // 128, 128), jnp.int32),
                    V((D, 8, H), f32), V((D, 8, H), f32), V((8, H), f32), V((8, H), f32),
                    V((DP, rows_dev), bf16), V((4, DP, rows_dev), bf16), V((4, rows_dev // 128, 128), jnp.int32),
                    V((DP, n_rows), f32), V((8, n_rows), f32),
                    V((GROUPS, 4 * HP, DP), f32), V((GROUPS, 4 * HP, 128), f32), V((GROUPS, 4 * HP, DP), f32), V((GROUPS, 4 * HP, 128), f32),
                    V((GROUPS, 8, n_rows), f32),
                    V((4, R, CHUNK), f32), V((4, R, CHUNK), f32), V((4, R, CHUNK), f32), V((GROUPS, R, 128), f32),
                    V((LEAD, R, CHUNK), f32), V((R, DP), f32),
                    V((2, 64, 128), f32), V((2, 64, 128), f32), V((4, 2, 64, 128), f32), V((4, 2, 64, 128), f32),
                    dma((6,)), dma((4,)), dma((4,)), dma((4,)), dma((4,)), dma((4, 2)), dma((4, 2)), dma((4, 2)), dma((4, 2)),
                ],
                compiler_params=pltpu.CompilerParams(collective_id=0, has_side_effects=True, vmem_limit_bytes=48 * 1024 * 1024),
            )(*[pltpu.with_memory_space_constraint(a, pltpu.HBM) for a in (x_rows.T, y_rows.reshape(rows_dev // 128, 128), wi, wo, mi, mo)])
            out = pl.pallas_call(
                store_kernel,
                name='store',
                out_shape=[S(o.shape, o.dtype) for o in out],
                in_specs=[vm] * 5,
                out_specs=[hbm] * 5,
                scratch_shapes=[dma((5,))],
                compiler_params=pltpu.CompilerParams(vmem_limit_bytes=4 * 1024 * 1024),
            )(*out)
            return out[0], out[1], out[2], out[3], out[4].reshape(-1)

        mapped = jax.shard_map(device_body, mesh=mesh, in_specs=(row_spec, label_spec, in_spec, out_spec, in_spec, out_spec),
                               out_specs=(in_spec, out_spec, in_spec, out_spec, chain_spec), check_vma=False)
        return mapped(feats, labels, w_in, w_out, mom_in, mom_out)

    return run_chains
```
